32 devices in a mesh: amp: 32 (over z, y, x, core).
Axes of the slice: x: 2, y: 2, z: 4, core: 2. Of those that a mesh axis runs over, the one named last changes fastest.
Arguments:
- ket_state: float32 [2, 1048576], P(None, 'amp'), may hold values from -6 to 6
- observable: float32 [1048576], P('amp'), may hold values from -6 to 6
- angles: float32 [2, 3], replicated, may hold values from -3.140625 to 3.140625
- gate_kinds: int32 [2, 32], replicated, may hold values from 0 to 2
Outputs:
- bra_state: float32 [2, 1048576], P(None, 'amp')
- grads: float32 [2, 3], replicated
The draws below stay inside these ranges and needn't reach their ends.
Inputs may be any that keep to these rules, and one draw needn't show every extreme that they name: `gate_kinds`: 0 and 1 name rotations about Y with angles[l, 0] and angles[l, 1], 2 a rotation about Z with angles[l, 2]; entries for qubits at or above the number of qubits are not used.
All inputs are finite; a program needn't handle non-finite values.
Results may differ from the reference program's by a relative error of at most 0.0003.
Values sent between devices are 32-bit elements; how exact they have to be, the bound alone decides.
A program may use at most 128 MiB of HBM per device.

```python
import math
import jax
import jax.numpy as jnp
from jax import lax

AMPS_DEV = 32768
LAYERS = 2
KINDS = 3
QSLOTS = 32
AMPS = 1048576
N_AMP = 32


def set_ends(drawn, own_key, smallest, largest):
    shape = drawn.shape
    place = [jax.random.randint(jax.random.fold_in(own_key, axis), (), 0, shape[axis]) for axis in range(len(shape))]
    drawn = drawn.at[tuple(place)].set(smallest)
    longest = shape.index(max(shape))
    place[longest] = (place[longest] + 1) % shape[longest]
    return drawn.at[tuple(place)].set(largest)


def block_levels(rng, dims, pieces, low, largest):
    def one(position, blocks):
        draws = jax.random.uniform(jax.random.fold_in(jax.random.fold_in(rng, 6), position), (blocks,), jnp.float32, low / len(pieces), largest / len(pieces))
        return jnp.repeat(jnp.exp(draws), dims[position] // blocks).reshape((-1,) + (1,) * (len(dims) - position - 1))

    factor_of = one(*pieces[0])
    for cut in pieces[1:]:
        factor_of = factor_of * one(*cut)
    return factor_of


def normal_values(stream_key, dims, spread, limit, cuts=(), kind=jnp.bfloat16):
    drawn = spread * jax.random.normal(stream_key, dims, jnp.float32)
    if cuts:
        drawn = drawn * block_levels(stream_key, dims, cuts, -0.22, 0.18)
    return jnp.clip(drawn, -limit, limit).astype(kind)


def setup_inputs(seed: int = 0) -> dict:
    streams_of = jax.random.split(jax.random.key(seed), 5)
    return {
        "ket_state": normal_values(streams_of[0], (2, AMPS), 1.0, 6.0, ((1, 32),), jnp.float32),
        "observable": normal_values(streams_of[1], (AMPS,), 1.0, 6.0, ((0, 32),), jnp.float32),
        "angles": jnp.clip(jax.random.uniform(streams_of[2], (LAYERS, KINDS), jnp.float32, -3.140625, 3.140625), -3.140625, 3.140625),
        "gate_kinds": set_ends(jax.random.randint(streams_of[3], (LAYERS, QSLOTS), 0, 3), jax.random.fold_in(streams_of[3], 1), 0, 2).astype(jnp.int32),
    }


def rotate_phase(values, cosine, sine_value):
    return jnp.stack([cosine * values[0] - sine_value * values[1], cosine * values[1] + sine_value * values[0]])

def undo_qubit(ket_state, bra_state, qubit_id, rotation, is_z):
    amp_total = ket_state.shape[1]
    fold_shape = (2, amp_total >> qubit_id + 1, 2, 1 << qubit_id)
    cosine = jnp.cos(0.5 * rotation)
    sine_value = jnp.sin(0.5 * rotation)

    def turn_y(operands):
        folded_ket, folded_bra = operands
        ket_low, ket_high = (folded_ket[:, :, 0], folded_ket[:, :, 1])
        bra_low, bra_high = (folded_bra[:, :, 0], folded_bra[:, :, 1])
        partial_value = 0.5 * jnp.sum(bra_high * ket_low - bra_low * ket_high)
        new_ket = jnp.stack([cosine * ket_low + sine_value * ket_high, cosine * ket_high - sine_value * ket_low], axis=2)
        new_bra = jnp.stack([cosine * bra_low + sine_value * bra_high, cosine * bra_high - sine_value * bra_low], axis=2)
        return (new_ket, new_bra, partial_value)

    def turn_z(operands):
        folded_ket, folded_bra = operands
        ket_low, ket_high = (folded_ket[:, :, 0], folded_ket[:, :, 1])
        bra_low, bra_high = (folded_bra[:, :, 0], folded_bra[:, :, 1])
        partial_value = 0.5 * (jnp.sum(bra_low[0] * ket_low[1] - bra_low[1] * ket_low[0]) - jnp.sum(bra_high[0] * ket_high[1] - bra_high[1] * ket_high[0]))
        new_ket = jnp.stack([rotate_phase(ket_low, cosine, sine_value), rotate_phase(ket_high, cosine, -sine_value)], axis=2)
        new_bra = jnp.stack([rotate_phase(bra_low, cosine, sine_value), rotate_phase(bra_high, cosine, -sine_value)], axis=2)
        return (new_ket, new_bra, partial_value)
    new_ket, new_bra, partial_value = lax.cond(is_z, turn_z, turn_y, (ket_state.reshape(fold_shape), bra_state.reshape(fold_shape)))
    return (new_ket.reshape(2, amp_total), new_bra.reshape(2, amp_total), partial_value)

def reference(ket_state, observable, angles, gate_kinds):
    amp_total = AMPS_DEV * N_AMP
    all_bits = int(amp_total).bit_length() - 1
    bra_state = 2.0 / math.sqrt(amp_total) * observable[None, :] * ket_state
    amp_index = jnp.arange(amp_total, dtype=jnp.int32)
    parity = jnp.zeros((amp_total,), jnp.int32)
    for qubit_id in range(all_bits):
        neighbor = (qubit_id + 1) % all_bits
        parity = parity + (amp_index >> qubit_id & 1) * (amp_index >> neighbor & 1)
    phase_sign = (1 - 2 * (parity & 1)).astype(jnp.float32)
    grads = jnp.zeros((LAYERS, KINDS), jnp.float32)
    kind_range = jnp.arange(KINDS)
    layer_range = jnp.arange(LAYERS)
    for layer_id in reversed(range(LAYERS)):
        ket_state = ket_state * phase_sign[None, :]
        bra_state = bra_state * phase_sign[None, :]
        for qubit_id in range(all_bits):
            kind_id = gate_kinds[layer_id, qubit_id]
            rotation = jnp.sum(jnp.where(kind_range == kind_id, angles[layer_id], 0.0))
            ket_state, bra_state, partial_value = undo_qubit(ket_state, bra_state, qubit_id, rotation, kind_id == 2)
            selector = ((layer_range[:, None] == layer_id) & (kind_range[None, :] == kind_id)).astype(grads.dtype)
            grads = grads + partial_value * selector
    return (bra_state, grads)
```

```python
import functools
import math

import jax
import jax.numpy as jnp
import numpy as np
from jax import lax
from jax.experimental import pallas as pl
from jax.experimental.pallas import tpu as pltpu
from jax.sharding import PartitionSpec as P

MESH = pl.DeviceIdType.MESH
LANE, SUB, MAJOR, DEVICE, CHUNK = range(5)
LANE_BITS, SUB_BITS = 7, 3
PLANES = 4


def from_partner(value, axis, apart):
    mask = 2**apart
    pairs = [(source, source ^ mask) for source in range(lax.axis_size(axis))]
    return lax.ppermute(value, axis, pairs)


def pair_tables():
    column = np.arange(128)
    flips = []
    signs = []
    for position in range(7):
        upper = column >> position & 1
        flip_table = np.zeros((128, 128), np.float32)
        flip_table[column, column ^ 1 << position] = np.where(upper == 0, -0.5, 0.5)
        flips.append(flip_table)
        signs.append((1 - 2 * upper).astype(np.float32))
    return (np.stack(flips), np.stack(signs))


def layout_map(local_bits, global_bits):
    local_map = list(range(local_bits))
    device_map = [local_bits + bit_num for bit_num in range(global_bits)]
    return (local_map, device_map)


def entangle_sign(local_bits, global_bits, device_id, amp_count):
    local_map, device_map = layout_map(local_bits, global_bits)
    amp_index = lax.iota(jnp.int32, amp_count)
    bit_values = [None] * (local_bits + global_bits)
    for position in range(local_bits):
        bit_values[local_map[position]] = amp_index >> position & 1
    for bit_num in range(global_bits):
        bit_values[device_map[bit_num]] = device_id >> bit_num & 1
    all_bits = local_bits + global_bits
    parity = jnp.zeros((amp_count,), jnp.int32)
    for qubit_id in range(all_bits):
        parity = parity + bit_values[qubit_id] * bit_values[(qubit_id + 1) % all_bits]
    return (1 - 2 * (parity & 1)).astype(jnp.float32)


def rotation_of(angles, gate_kinds, layer_id, qubit_id):
    kind_id = gate_kinds[layer_id, qubit_id]
    chosen = jnp.arange(angles.shape[1]) == kind_id
    rotation = jnp.sum(jnp.where(chosen, angles[layer_id], 0.0))
    return (kind_id, jnp.cos(0.5 * rotation), jnp.sin(0.5 * rotation))


def kind_vector(kind_id, kind_count):
    return (jnp.arange(kind_count) == kind_id).astype(jnp.float32)


def rotate_phase(values, cosine, sine_value):
    return jnp.stack(
        [cosine * values[0] - sine_value * values[1], cosine * values[1] + sine_value * values[0]]
    )


def rotate_position(ket_state, bra_state, position, qubit_id, layer_id, angles, gate_kinds):
    amp_count = ket_state.shape[1]
    fold_shape = (2, amp_count >> position + 1, 2, 1 << position)
    kind_id, cosine, sine_value = rotation_of(angles, gate_kinds, layer_id, qubit_id)

    def turn_y(operands):
        folded_ket, folded_bra = operands
        ket_low, ket_high = (folded_ket[:, :, 0], folded_ket[:, :, 1])
        bra_low, bra_high = (folded_bra[:, :, 0], folded_bra[:, :, 1])
        partial_value = 0.5 * jnp.sum(bra_high * ket_low - bra_low * ket_high)
        new_ket = jnp.stack(
            [cosine * ket_low + sine_value * ket_high, cosine * ket_high - sine_value * ket_low],
            axis=2,
        )
        new_bra = jnp.stack(
            [cosine * bra_low + sine_value * bra_high, cosine * bra_high - sine_value * bra_low],
            axis=2,
        )
        return (new_ket, new_bra, partial_value)

    def turn_z(operands):
        folded_ket, folded_bra = operands
        ket_low, ket_high = (folded_ket[:, :, 0], folded_ket[:, :, 1])
        bra_low, bra_high = (folded_bra[:, :, 0], folded_bra[:, :, 1])
        partial_value = 0.5 * (
            jnp.sum(bra_low[0] * ket_low[1] - bra_low[1] * ket_low[0])
            - jnp.sum(bra_high[0] * ket_high[1] - bra_high[1] * ket_high[0])
        )
        new_ket = jnp.stack(
            [
                rotate_phase(ket_low, cosine, sine_value),
                rotate_phase(ket_high, cosine, -sine_value),
            ],
            axis=2,
        )
        new_bra = jnp.stack(
            [
                rotate_phase(bra_low, cosine, sine_value),
                rotate_phase(bra_high, cosine, -sine_value),
            ],
            axis=2,
        )
        return (new_ket, new_bra, partial_value)

    new_ket, new_bra, partial_value = lax.cond(
        kind_id == 2, turn_z, turn_y, (ket_state.reshape(fold_shape), bra_state.reshape(fold_shape))
    )
    terms = partial_value * kind_vector(kind_id, angles.shape[1])
    return (new_ket.reshape(2, amp_count), new_bra.reshape(2, amp_count), terms)


def contract_rows(left, right):
    return lax.dot_general(
        left,
        right,
        (((0,), (0,)), ((), ())),
        precision=lax.Precision.HIGHEST,
        preferred_element_type=jnp.float32,
    )


def contract_cols(left, right):
    return lax.dot_general(
        left,
        right,
        (((1,), (1,)), ((), ())),
        precision=lax.Precision.HIGHEST,
        preferred_element_type=jnp.float32,
    )


def low_block(ket_state, bra_state, qubit_list, layer_id, angles, gate_kinds):
    amp_count = ket_state.shape[1]
    row_count = amp_count // 128
    flips, signs = pair_tables()
    ket_real = ket_state[0].reshape(row_count, 128)
    ket_imag = ket_state[1].reshape(row_count, 128)
    bra_real = bra_state[0].reshape(row_count, 128)
    bra_imag = bra_state[1].reshape(row_count, 128)
    gram_real = contract_rows(bra_real, ket_real) + contract_rows(bra_imag, ket_imag)
    gram_imag = contract_rows(bra_real, ket_imag) - contract_rows(bra_imag, ket_real)
    gram_diag = jnp.diagonal(gram_imag)
    terms = jnp.zeros((angles.shape[1],), jnp.float32)
    kron_real = None
    kron_imag = None
    for position in range(7):
        kind_id, cosine, sine_value = rotation_of(
            angles, gate_kinds, layer_id, qubit_list[position]
        )
        is_z = kind_id == 2
        partial_value = jnp.where(
            is_z, 0.5 * jnp.sum(signs[position] * gram_diag), jnp.sum(flips[position] * gram_real)
        )
        terms = terms + partial_value * kind_vector(kind_id, angles.shape[1])
        mat_y = jnp.stack([jnp.stack([cosine, sine_value]), jnp.stack([-sine_value, cosine])])
        zero_value = jnp.zeros_like(cosine)
        mat_zr = jnp.stack([jnp.stack([cosine, zero_value]), jnp.stack([zero_value, cosine])])
        mat_zi = jnp.stack(
            [jnp.stack([sine_value, zero_value]), jnp.stack([zero_value, -sine_value])]
        )
        mat_real = jnp.where(is_z, mat_zr, mat_y)
        mat_imag = jnp.where(is_z, mat_zi, jnp.zeros_like(mat_zi))
        if kron_real is None:
            kron_real, kron_imag = (mat_real, mat_imag)
        else:
            kron_real, kron_imag = (
                jnp.kron(mat_real, kron_real) - jnp.kron(mat_imag, kron_imag),
                jnp.kron(mat_real, kron_imag) + jnp.kron(mat_imag, kron_real),
            )

    def apply_block(real_rows, imag_rows):
        new_real = contract_cols(real_rows, kron_real) - contract_cols(imag_rows, kron_imag)
        new_imag = contract_cols(imag_rows, kron_real) + contract_cols(real_rows, kron_imag)
        return jnp.stack([new_real.reshape(amp_count), new_imag.reshape(amp_count)])

    return (apply_block(ket_real, ket_imag), apply_block(bra_real, bra_imag), terms)


def rotate_global(
    ket_state,
    bra_state,
    far_ket,
    far_bra,
    bit_num,
    qubit_id,
    device_id,
    layer_id,
    angles,
    gate_kinds,
):
    kind_id, cosine, sine_value = rotation_of(angles, gate_kinds, layer_id, qubit_id)
    orient = (1 - 2 * (device_id >> bit_num & 1)).astype(jnp.float32)

    def turn_y(operands):
        own_ket, own_bra, other_ket, other_bra = operands
        partial_value = 0.25 * orient * jnp.sum(other_bra * own_ket - own_bra * other_ket)
        return (
            cosine * own_ket + orient * sine_value * other_ket,
            cosine * own_bra + orient * sine_value * other_bra,
            partial_value,
        )

    def turn_z(operands):
        own_ket, own_bra, other_ket, other_bra = operands
        partial_value = 0.5 * orient * jnp.sum(own_bra[0] * own_ket[1] - own_bra[1] * own_ket[0])
        return (
            rotate_phase(own_ket, cosine, orient * sine_value),
            rotate_phase(own_bra, cosine, orient * sine_value),
            partial_value,
        )

    new_ket, new_bra, partial_value = lax.cond(
        kind_id == 2, turn_z, turn_y, (ket_state, bra_state, far_ket, far_bra)
    )
    return (new_ket, new_bra, partial_value * kind_vector(kind_id, angles.shape[1]))


def on_device(ket_state, observable, angles, gate_kinds):
    amp_count = ket_state.shape[1]
    local_bits = amp_count.bit_length() - 1
    group_size = lax.axis_size("amp")
    global_bits = group_size.bit_length() - 1
    device_id = lax.axis_index("amp")
    layer_count = angles.shape[0]
    kind_count = angles.shape[1]
    bra_state = 2.0 / math.sqrt(amp_count * group_size) * observable[None, :] * ket_state
    sign_cache = {}
    grads_local = jnp.zeros((layer_count, kind_count), jnp.float32)
    for sweep_id in range(layer_count):
        layer_id = layer_count - 1 - sweep_id
        layout = 0
        local_map, device_map = layout_map(local_bits, global_bits)
        if layout not in sign_cache:
            sign_cache[layout] = entangle_sign(local_bits, global_bits, device_id, amp_count)
        phase_sign = sign_cache[layout]
        ket_state = ket_state * phase_sign[None, :]
        bra_state = bra_state * phase_sign[None, :]
        ket_state, bra_state, layer_terms = low_block(
            ket_state, bra_state, local_map[:7], layer_id, angles, gate_kinds
        )
        for position in range(7, local_bits):
            ket_state, bra_state, partial_value = rotate_position(
                ket_state, bra_state, position, local_map[position], layer_id, angles, gate_kinds
            )
            layer_terms = layer_terms + partial_value
        for bit_num in range(global_bits):
            far_ket, far_bra = from_partner((ket_state, bra_state), "amp", bit_num)
            ket_state, bra_state, partial_value = rotate_global(
                ket_state,
                bra_state,
                far_ket,
                far_bra,
                bit_num,
                device_map[bit_num],
                device_id,
                layer_id,
                angles,
                gate_kinds,
            )
            layer_terms = layer_terms + partial_value
        grads_local = grads_local.at[layer_id].set(layer_terms)
    grads = lax.psum(grads_local, "amp")
    return (bra_state, grads)


def chunk_layouts(g):
    top = g + LANE_BITS + SUB_BITS - 1
    home, away = {}, {}
    for q in range(LANE_BITS):
        home[q] = away[q] = (LANE, q)
    for bit, q in ((1, top - 1), (2, top)):
        home[q] = away[q] = (SUB, bit)
    moved = list(range(LANE_BITS + 2, top - 1)) + [LANE_BITS]
    for bit, q in enumerate(moved):
        home[q], away[q] = (MAJOR, bit), (DEVICE, bit)
    home[LANE_BITS + 1], away[LANE_BITS + 1] = (MAJOR, g), (CHUNK, 0)
    for bit in range(g):
        home[top + 1 + bit], away[top + 1 + bit] = (DEVICE, bit), (MAJOR, bit)
    return home, away


def split_major(x, bit):
    fold = x.reshape((x.shape[0] >> bit + 1, 2, 1 << bit) + x.shape[1:])
    return fold[:, 0], fold[:, 1]


def join_major(x0, x1):
    out = jnp.stack([x0, x1], axis=1)
    return out.reshape((-1,) + out.shape[3:])


def minor_bit(axis, bit):
    return lax.broadcasted_iota(jnp.int32, (1, 8, 128), 1 if axis == SUB else 2) >> bit & 1


def minor_sign(axis, bit):
    return (1 - 2 * minor_bit(axis, bit)).astype(jnp.float32)


def shifted(x, axis, by):
    dim = 1 if axis == SUB else 2
    return pltpu.roll(x, by % x.shape[dim], dim)


def partner(x, axis, bit):
    step = 1 << bit
    up = shifted(x, axis, -step)
    if 2 * step == x.shape[1 if axis == SUB else 2]:
        return up
    return jnp.where(minor_bit(axis, bit) == 0, up, shifted(x, axis, step))


def swap_bits(x, major, sub):
    x0, x1 = split_major(x, major)
    lower = minor_bit(SUB, sub) == 0

    def roll3(y, by):
        z = y.reshape((-1,) + y.shape[2:])
        return shifted(z, SUB, by).reshape(y.shape)

    step = 1 << sub
    return join_major(jnp.where(lower, x0, roll3(x1, step)), jnp.where(lower, roll3(x0, -step), x1))


def other_part(x):
    return partner(x, SUB, 0)


def weights(obs, chunk):
    place = lax.broadcasted_iota(jnp.int32, (1, 8, 128), 1) & 3
    if chunk == 0:
        end, far = 0, 3
    else:
        end, far = 3, 0
    step = 1 if chunk == 0 else -1
    near = jnp.where(place == end, obs, shifted(obs, SUB, step))
    return jnp.where(place == far, shifted(obs, SUB, 2 * step), near)


def y_gate(x, place, cy, sy):
    axis, bit = place
    if axis == MAJOR:
        x0, x1 = split_major(x, bit)
        return join_major(cy * x0 + sy * x1, cy * x1 - sy * x0)
    return cy * x + (sy * minor_sign(axis, bit)) * partner(x, axis, bit)


def lane_matrix(coefs):
    at = [lax.broadcasted_iota(jnp.int32, (128, 128), d) for d in range(2)]
    re, im = None, None
    for bit, (c, sy, sz) in enumerate(coefs):
        old, new = (x >> bit & 1 for x in at)
        z = (1 - 2 * new).astype(jnp.float32)
        same = old == new
        a, b = jnp.where(same, c, sy * z), jnp.where(same, sz * z, 0.0)
        re, im = (a, b) if re is None else (re * a - im * b, re * b + im * a)
    return jnp.concatenate([re, im], 1)


def turn_lanes(x, matrix):
    both = lax.dot_general(
        x.reshape(-1, 128),
        matrix[...],
        (((1,), (0,)), ((), ())),
        precision=lax.Precision.HIGH,
        preferred_element_type=jnp.float32,
    )
    re, im = both[:, :128].reshape(x.shape), both[:, 128:].reshape(x.shape)
    return re - minor_sign(SUB, 0) * other_part(im)


def terms(bra, ket, place, w, w_sum):
    axis, bit = place
    if axis == MAJOR:
        b0, b1 = split_major(bra, bit)
        k0, k1 = split_major(ket, bit)
        w0, w1 = split_major(w, bit)
        return 0.5 * jnp.sum(b1 * k0 - b0 * k1, axis=(0, 1)), 0.5 * jnp.sum(w0 - w1, axis=(0, 1))
    z = 0.5 * minor_sign(axis, bit)[0]
    return -z * jnp.sum(bra * partner(ket, axis, bit), axis=0), z * w_sum


def phases(place, qubits, edges, majors, me, chunk, turns=None):
    def bit_of(q):
        axis, bit = place[q]
        if axis in (LANE, SUB):
            return minor_bit(axis, bit)
        return me >> bit & 1 if axis == DEVICE else chunk

    at_major = {place[q][1]: q for q in range(qubits) if place[q][0] == MAJOR}
    parity = jnp.zeros((1, 8, 128), jnp.int32)
    for q in edges:
        ends = (q, (q + 1) % qubits)
        if all(place[e][0] != MAJOR for e in ends):
            parity = parity + bit_of(ends[0]) * bit_of(ends[1])
    re = (1 - 2 * (parity & 1)).astype(jnp.float32)
    im = None

    def times(re, im, c, s):
        if im is None:
            return re * c, re * s
        return re * c - im * s, im * c + re * s

    turns = turns or {}
    for q, (c, s) in turns.items():
        axis, bit = place[q]
        if axis != MAJOR:
            re, im = times(re, im, c, s * minor_sign(axis, bit))
    for j in range(majors.bit_length() - 1):
        q = at_major[j]
        parity, flips = None, []
        for edge, o in ((q, (q + 1) % qubits), ((q - 1) % qubits, (q - 1) % qubits)):
            if edge not in edges:
                continue
            if place[o][0] != MAJOR:
                parity = bit_of(o) if parity is None else parity + bit_of(o)
            elif place[o][1] < j:
                flips.append(place[o][1])

        def upper(x):
            if parity is not None:
                x = x * jnp.broadcast_to(1 - 2 * (parity & 1), (1, 8, 128)).astype(jnp.float32)
            for bit in flips:
                x0, x1 = split_major(x, bit)
                x = join_major(x0, -x1)
            return x

        lo, hi = (re, im), (upper(re), None if im is None else upper(im))
        if q in turns:
            c, s = turns[q]
            lo, hi = times(*lo, c, s), times(*hi, c, -s)
        re = jnp.concatenate([lo[0], hi[0]], 0)
        im = None if lo[1] is None else jnp.concatenate([lo[1], hi[1]], 0)
    return (re, None) if im is None else (re, -minor_sign(SUB, 0) * im)


def half_turn(angle):
    x = 0.5 * angle
    x2 = x * x
    cosine, sine = 0.0, 0.0
    for n in range(8, -1, -1):
        cosine = cosine * x2 + (-1.0) ** n / math.factorial(2 * n)
        sine = sine * x2 + (-1.0) ** n / math.factorial(2 * n + 1)
    return cosine, sine * x


def kernel(
    n, qubits, angles, kinds, ket_ref, obs_ref, out_ref, grads_ref,
    ket_in, obs_in, sent, held, back, landed, gsent, gheld, gsent2, gheld2,
    flag, send1, recv1, send2, recv2, gsend, grecv, gsend2, grecv2, load, wide,
):
    me = lax.axis_index("amp")
    g = n.bit_length() - 1
    home, away = chunk_layouts(g)
    scale = 2.0 / math.sqrt(2**qubits)

    loads = [
        pltpu.make_async_copy(ket_ref, ket_in, load.at[0]),
        pltpu.make_async_copy(obs_ref, obs_in, load.at[1]),
    ]
    for copy in loads:
        copy.start()

    half, size = n // 2, n // PLANES
    plane, place = me // size, me % size
    upper = plane // 2
    near = 2 - upper
    far = near + 1 - 2 * upper
    side = plane + 1 - 2 * (plane % 2)
    others = (near, far, side)

    def inside(j):
        spot = place
        for bit in range(size.bit_length() - 1):
            if j >> bit & 1:
                spot = spot + (1 - 2 * (place // (1 << bit) % 2)) * (1 << bit)
        return spot

    spots = [inside(j) for j in range(size)]
    barrier = pltpu.get_barrier_semaphore()
    for other in others:
        pl.semaphore_signal(barrier, inc=1, device_id=(other * size + place,), device_id_type=MESH)
    for spot in spots[1:]:
        pl.semaphore_signal(barrier, inc=1, device_id=(plane * size + spot,), device_id_type=MESH)
    for copy in loads:
        copy.wait()

    value = ket_in[...].reshape(2 * n, 8, 128)
    for bit in (1, 2):
        value = swap_bits(value, g - 2 + bit, bit)
    sent[:, 0] = value[:n]
    sent[:, 1] = value[n:]
    value = obs_in[...].reshape(n, 8, 128)
    for major, bit in ((g - 2, 0), (g - 1, 2)):
        value = swap_bits(value, major, bit)
    sent[:, 2] = jnp.stack([value[:half], value[half:]], axis=1).reshape(n, 8, 128)

    pl.semaphore_wait(barrier, size - 1 + len(others))
    for other in others:
        pl.semaphore_signal(flag.at[plane], inc=1, device_id=(other * size + place,), device_id_type=MESH)

    def exchange(source, target, send, recv):
        def copy(block):
            return pltpu.make_async_remote_copy(
                src_ref=source.at[block],
                dst_ref=target.at[me],
                send_sem=send,
                recv_sem=recv.at[plane],
                device_id=(block,),
                device_id_type=MESH,
            )

        def start(to, picked):
            for spot in picked:
                copy(to * size + spot).start()

        def many(first, count, origin):
            return pltpu.make_async_remote_copy(
                src_ref=source.at[pl.ds(first, count)],
                dst_ref=target.at[pl.ds(first, count)],
                send_sem=send,
                recv_sem=recv.at[origin],
                device_id=(me,),
                device_id_type=MESH,
            )

        def arrive(origin):
            count = size - 1 if origin is plane else size
            many(origin * size, count, origin).wait_recv()

        def depart():
            many(0, n - 1, plane).wait_send()

        return start, arrive, depart

    def gather(source, target, send, recv, stride, count):
        digit = me // stride % count

        def copies():
            for k in range(1, count):
                yield pltpu.make_async_remote_copy(
                    src_ref=source,
                    dst_ref=target.at[k],
                    send_sem=send.at[k],
                    recv_sem=recv.at[k],
                    device_id=(me + ((digit + k) % count - digit) * stride,),
                    device_id_type=MESH,
                )

        target[0] = source[...]
        for copy in copies():
            copy.start()
        return lambda: [copy.wait_recv() for copy in copies()], lambda: [copy.wait_send() for copy in copies()]

    start1, arrive1, depart1 = exchange(sent, held, send1, recv1)
    start2, arrive2, depart2 = exchange(back, landed, send2, recv2)
    start1(far, spots[:1])
    start1(near, spots[:1])
    start1(plane, spots[:0:-1])
    start1(side, spots[:1])
    for other in others:
        pl.semaphore_wait(flag.at[other], 1)
        start1(other, spots[:0:-1])
    held[me] = sent[me]

    layers, kind_count = angles.shape
    turns = [[half_turn(angles[l, k]) for k in range(kind_count)] for l in range(layers)]
    coefs, shares = [], []
    for l in range(layers):
        row, share = [], []
        for q in range(qubits):
            kind = kinds[l, q]
            is_kind = [jnp.where(kind == k, 1.0, 0.0) for k in range(kind_count)]
            cy = sum(is_kind[k] * turns[l][k][0] for k in range(kind_count - 1))
            sy = sum(is_kind[k] * turns[l][k][1] for k in range(kind_count - 1))
            cz = is_kind[-1] * turns[l][-1][0]
            sz = is_kind[-1] * turns[l][-1][1]
            row.append((cy + is_kind[-1], sy, cz + (1.0 - is_kind[-1]), sz, cy + cz))
            share.append(is_kind)
        coefs.append(row)
        shares.append(share)

    every = range(qubits)
    late = [q for q in every if home[q][0] == MAJOR]
    first, last = min(late), max(late)
    late_edges = [q for q in every if first - 1 <= q <= last]
    early_edges = [q for q in every if q not in late_edges]
    local = [q for q in every if home[q][0] != DEVICE]
    outer = [q for q in every if home[q][0] == DEVICE]
    here = [q for q in every if q not in late]
    ready = [q for q in here if q not in (first - 1, last + 1)]
    rest = [q for q in local if q not in ready]

    for l in range(layers):
        lanes = [
            (coefs[l][q][4], coefs[l][q][1], coefs[l][q][3]) if l == 1 or q in ready else (1.0, 0.0, 0.0)
            for q in range(LANE_BITS)
        ]
        wide[l] = lane_matrix(lanes)

    sums = [[jnp.zeros((8, 128), jnp.float32) for _ in range(kind_count)] for _ in range(layers)]

    def add_terms(l, chosen, place, bra, ket):
        w = minor_sign(SUB, 0) * (bra * other_part(ket))
        w_sum = jnp.sum(w, axis=0)
        for q in chosen:
            y, z = terms(bra, ket, place[q], w, w_sum)
            for k in range(kind_count):
                sums[l][k] = sums[l][k] + shares[l][q][k] * (z if k == kind_count - 1 else y)

    def phase_of(l, chosen, place, edges, majors, chunk, by_matrix):
        turned = {q: coefs[l][q][2:4] for q in chosen if not (by_matrix and place[q][0] == LANE)}
        return phases(place, qubits, edges, majors, me, chunk, turned)

    def turn(x, l, chosen, place, phase, by_matrix=True):
        if by_matrix:
            x = turn_lanes(x, wide.at[l])
        for q in chosen:
            if not (by_matrix and place[q][0] == LANE):
                x = y_gate(x, place[q], coefs[l][q][0], coefs[l][q][1])
        return phase[0] * x + phase[1] * other_part(x)

    sign, _ = phases(home, qubits, every, 2 * n, me, 0)
    phase = phase_of(1, local, home, every, 2 * n, 0, True)
    ket = jnp.concatenate([sent[:, 0], sent[:, 1]], 0) * sign
    obs = sent[:, 2]
    bra = scale * jnp.concatenate([weights(obs, 0), weights(obs, 1)], 0) * ket
    add_terms(1, local, home, bra, ket)
    ket, bra = (turn(x, 1, local, home, phase) for x in (ket, bra))
    add_terms(0, local[1:-1], home, bra, ket)

    ready_phase = phase_of(0, ready, away, [], n, 0, True)
    signs = [phases(away, qubits, every, n, me, chunk)[0] for chunk in range(2)]
    mid_phases = [phase_of(1, here, away, early_edges, n, chunk, True) for chunk in range(2)]
    for origin in (plane,) + others:
        arrive1(origin)
    states = []
    for chunk in range(2):
        ket = held[:, chunk] * signs[chunk]
        bra = scale * weights(held[:, 2], chunk) * ket
        bra_mid = turn(bra, 1, here, away, mid_phases[chunk])
        back[:, chunk] = turn(bra_mid, 0, ready, away, ready_phase)
        states.append((ket, bra, bra_mid))
    for other in (far, near, side):
        start2(other, spots[::-1])
    start2(plane, spots[:0:-1])
    landed[me] = back[me]
    for chunk, (ket, bra, bra_mid) in enumerate(states):
        add_terms(1, outer, away, bra, ket)
        ket = turn(ket, 1, here, away, mid_phases[chunk])
        add_terms(0, [local[-1]] + outer + [0], away, bra_mid, ket)

    at = [lax.broadcasted_iota(jnp.int32, (layers, 128), d) for d in range(2)]
    total = jnp.zeros((layers, 128), jnp.float32)
    for l in range(layers):
        for k in range(kind_count):
            total = total + jnp.where((at[0] == l) & (at[1] == k), jnp.sum(sums[l][k]), 0.0)
    inner = gheld.shape[0]
    gsent[...] = total
    garrive, gdepart = gather(gsent, gheld, gsend, grecv, 1, inner)
    garrive()
    gsent2[...] = jnp.sum(gheld[...], axis=0)
    garrive2, gdepart2 = gather(gsent2, gheld2, gsend2, grecv2, inner, n // inner)

    late_phase = phase_of(1, late, home, late_edges, 2 * n, 0, False)
    rest_phase = phase_of(0, rest, home, [], 2 * n, 0, False)
    for origin in (plane,) + others:
        arrive2(origin)
    x = jnp.concatenate([landed[:, 0], landed[:, 1]], 0)
    x = turn(x, 1, late, home, late_phase, False)
    x = turn(x, 0, rest, home, rest_phase, False)
    for bit in (1, 2):
        x = swap_bits(x, g - 2 + bit, bit)
    out_ref[...] = x.reshape(16 * n, 128)
    garrive2()
    grads_ref[...] = jnp.sum(gheld2[...], axis=0)
    depart1()
    depart2()
    gdepart()
    gdepart2()


def finish(bra_ref, sums_ref, out_ref, grads_ref, sem):
    copy = pltpu.make_async_copy(bra_ref, out_ref, sem)
    copy.start()
    grads_ref[...] = sums_ref[:, : grads_ref.shape[1]]
    copy.wait()


def by_exchange(ket_state, observable, angles, gate_kinds):
    amp_count = ket_state.shape[1]
    n = lax.axis_size("amp")
    qubits = (amp_count * n).bit_length() - 1
    layers, kind_count = angles.shape
    rows = amp_count // 128
    ket = ket_state.reshape(2, rows, 128).transpose(1, 0, 2).reshape(2 * rows, 128)
    vmem = pl.BlockSpec(memory_space=pltpu.VMEM)
    smem = pl.BlockSpec(memory_space=pltpu.SMEM)
    hbm = pl.BlockSpec(memory_space=pltpu.HBM)
    inner = 1 << n.bit_length() // 2
    outer = n // inner
    f32 = jnp.float32
    dma = pltpu.SemaphoreType.DMA
    bra, sums = pl.pallas_call(
        functools.partial(kernel, n, qubits),
        out_shape=(
            pltpu.VMEM((2 * rows, 128), f32),
            pltpu.VMEM((layers, 128), f32),
        ),
        in_specs=[smem, smem, hbm, hbm],
        out_specs=(vmem, vmem),
        scratch_shapes=[
            pltpu.VMEM((2 * rows, 128), f32),
            pltpu.VMEM((rows, 128), f32),
            pltpu.VMEM((n, 3, 8, 128), f32),
            pltpu.VMEM((n, 3, 8, 128), f32),
            pltpu.VMEM((n, 2, 8, 128), f32),
            pltpu.VMEM((n, 2, 8, 128), f32),
            pltpu.VMEM((layers, 128), f32),
            pltpu.VMEM((inner, layers, 128), f32),
            pltpu.VMEM((layers, 128), f32),
            pltpu.VMEM((outer, layers, 128), f32),
            pltpu.SemaphoreType.REGULAR((PLANES,)),
            dma,
            dma((PLANES,)),
            dma,
            dma((PLANES,)),
        ]
        + [dma((size,)) for size in (inner, inner, outer, outer, 2)]
        + [pltpu.VMEM((layers, 128, 256), f32)],
        compiler_params=pltpu.CompilerParams(
            collective_id=0, has_side_effects=True
        ),
    )(angles, gate_kinds, *(pltpu.with_memory_space_constraint(x, pltpu.HBM) for x in (ket, observable.reshape(rows, 128))))
    out, grads = pl.pallas_call(
        finish,
        out_shape=(
            jax.ShapeDtypeStruct((2 * rows, 128), f32),
            jax.ShapeDtypeStruct((layers, kind_count), f32),
        ),
        in_specs=[vmem, vmem],
        out_specs=(hbm, vmem),
        scratch_shapes=[dma],
        compiler_params=pltpu.CompilerParams(vmem_limit_bytes=1 << 20),
    )(*(pltpu.with_memory_space_constraint(x, pltpu.VMEM) for x in (bra, sums)))
    bra_state = out.reshape(rows, 2, 128).transpose(1, 0, 2).reshape(2, amp_count)
    return (bra_state, grads)


def per_device(ket_state, observable, angles, gate_kinds):
    tiles = ket_state.shape[1] // (1 << LANE_BITS + SUB_BITS)
    if tiles == lax.axis_size("amp") and tiles >= 8 and angles.shape == (2, 3):
        return by_exchange(ket_state, observable, angles, gate_kinds)
    return on_device(ket_state, observable, angles, gate_kinds)


def solution(mesh):
    placed = (P(None, "amp"), P("amp"), P(), P())
    return jax.shard_map(
        per_device, mesh=mesh, in_specs=placed, out_specs=(P(None, "amp"), P()), check_vma=False
    )
```

```python
import functools
import math

import jax
import jax.numpy as jnp
import numpy as np
from jax import lax
from jax.experimental import pallas as pl
from jax.experimental.pallas import tpu as pltpu
from jax.sharding import PartitionSpec as P

MESH = pl.DeviceIdType.MESH
LANE, SUB, MAJOR, DEVICE, CHUNK = range(5)
LANE_BITS, SUB_BITS = 7, 3
PLANES = 4


def from_partner(value, axis, apart):
    mask = 2**apart
    pairs = [(source, source ^ mask) for source in range(lax.axis_size(axis))]
    return lax.ppermute(value, axis, pairs)


def pair_tables():
    column = np.arange(128)
    flips = []
    signs = []
    for position in range(7):
        upper = column >> position & 1
        flip_table = np.zeros((128, 128), np.float32)
        flip_table[column, column ^ 1 << position] = np.where(upper == 0, -0.5, 0.5)
        flips.append(flip_table)
        signs.append((1 - 2 * upper).astype(np.float32))
    return (np.stack(flips), np.stack(signs))


def layout_map(local_bits, global_bits):
    local_map = list(range(local_bits))
    device_map = [local_bits + bit_num for bit_num in range(global_bits)]
    return (local_map, device_map)


def entangle_sign(local_bits, global_bits, device_id, amp_count):
    local_map, device_map = layout_map(local_bits, global_bits)
    amp_index = lax.iota(jnp.int32, amp_count)
    bit_values = [None] * (local_bits + global_bits)
    for position in range(local_bits):
        bit_values[local_map[position]] = amp_index >> position & 1
    for bit_num in range(global_bits):
        bit_values[device_map[bit_num]] = device_id >> bit_num & 1
    all_bits = local_bits + global_bits
    parity = jnp.zeros((amp_count,), jnp.int32)
    for qubit_id in range(all_bits):
        parity = parity + bit_values[qubit_id] * bit_values[(qubit_id + 1) % all_bits]
    return (1 - 2 * (parity & 1)).astype(jnp.float32)


def rotation_of(angles, gate_kinds, layer_id, qubit_id):
    kind_id = gate_kinds[layer_id, qubit_id]
    chosen = jnp.arange(angles.shape[1]) == kind_id
    rotation = jnp.sum(jnp.where(chosen, angles[layer_id], 0.0))
    return (kind_id, jnp.cos(0.5 * rotation), jnp.sin(0.5 * rotation))


def kind_vector(kind_id, kind_count):
    return (jnp.arange(kind_count) == kind_id).astype(jnp.float32)


def rotate_phase(values, cosine, sine_value):
    return jnp.stack(
        [cosine * values[0] - sine_value * values[1], cosine * values[1] + sine_value * values[0]]
    )


def rotate_position(ket_state, bra_state, position, qubit_id, layer_id, angles, gate_kinds):
    amp_count = ket_state.shape[1]
    fold_shape = (2, amp_count >> position + 1, 2, 1 << position)
    kind_id, cosine, sine_value = rotation_of(angles, gate_kinds, layer_id, qubit_id)

    def turn_y(operands):
        folded_ket, folded_bra = operands
        ket_low, ket_high = (folded_ket[:, :, 0], folded_ket[:, :, 1])
        bra_low, bra_high = (folded_bra[:, :, 0], folded_bra[:, :, 1])
        partial_value = 0.5 * jnp.sum(bra_high * ket_low - bra_low * ket_high)
        new_ket = jnp.stack(
            [cosine * ket_low + sine_value * ket_high, cosine * ket_high - sine_value * ket_low],
            axis=2,
        )
        new_bra = jnp.stack(
            [cosine * bra_low + sine_value * bra_high, cosine * bra_high - sine_value * bra_low],
            axis=2,
        )
        return (new_ket, new_bra, partial_value)

    def turn_z(operands):
        folded_ket, folded_bra = operands
        ket_low, ket_high = (folded_ket[:, :, 0], folded_ket[:, :, 1])
        bra_low, bra_high = (folded_bra[:, :, 0], folded_bra[:, :, 1])
        partial_value = 0.5 * (
            jnp.sum(bra_low[0] * ket_low[1] - bra_low[1] * ket_low[0])
            - jnp.sum(bra_high[0] * ket_high[1] - bra_high[1] * ket_high[0])
        )
        new_ket = jnp.stack(
            [
                rotate_phase(ket_low, cosine, sine_value),
                rotate_phase(ket_high, cosine, -sine_value),
            ],
            axis=2,
        )
        new_bra = jnp.stack(
            [
                rotate_phase(bra_low, cosine, sine_value),
                rotate_phase(bra_high, cosine, -sine_value),
            ],
            axis=2,
        )
        return (new_ket, new_bra, partial_value)

    new_ket, new_bra, partial_value = lax.cond(
        kind_id == 2, turn_z, turn_y, (ket_state.reshape(fold_shape), bra_state.reshape(fold_shape))
    )
    terms = partial_value * kind_vector(kind_id, angles.shape[1])
    return (new_ket.reshape(2, amp_count), new_bra.reshape(2, amp_count), terms)


def contract_rows(left, right):
    return lax.dot_general(
        left,
        right,
        (((0,), (0,)), ((), ())),
        precision=lax.Precision.HIGHEST,
        preferred_element_type=jnp.float32,
    )


def contract_cols(left, right):
    return lax.dot_general(
        left,
        right,
        (((1,), (1,)), ((), ())),
        precision=lax.Precision.HIGHEST,
        preferred_element_type=jnp.float32,
    )


def low_block(ket_state, bra_state, qubit_list, layer_id, angles, gate_kinds):
    amp_count = ket_state.shape[1]
    row_count = amp_count // 128
    flips, signs = pair_tables()
    ket_real = ket_state[0].reshape(row_count, 128)
    ket_imag = ket_state[1].reshape(row_count, 128)
    bra_real = bra_state[0].reshape(row_count, 128)
    bra_imag = bra_state[1].reshape(row_count, 128)
    gram_real = contract_rows(bra_real, ket_real) + contract_rows(bra_imag, ket_imag)
    gram_imag = contract_rows(bra_real, ket_imag) - contract_rows(bra_imag, ket_real)
    gram_diag = jnp.diagonal(gram_imag)
    terms = jnp.zeros((angles.shape[1],), jnp.float32)
    kron_real = None
    kron_imag = None
    for position in range(7):
        kind_id, cosine, sine_value = rotation_of(
            angles, gate_kinds, layer_id, qubit_list[position]
        )
        is_z = kind_id == 2
        partial_value = jnp.where(
            is_z, 0.5 * jnp.sum(signs[position] * gram_diag), jnp.sum(flips[position] * gram_real)
        )
        terms = terms + partial_value * kind_vector(kind_id, angles.shape[1])
        mat_y = jnp.stack([jnp.stack([cosine, sine_value]), jnp.stack([-sine_value, cosine])])
        zero_value = jnp.zeros_like(cosine)
        mat_zr = jnp.stack([jnp.stack([cosine, zero_value]), jnp.stack([zero_value, cosine])])
        mat_zi = jnp.stack(
            [jnp.stack([sine_value, zero_value]), jnp.stack([zero_value, -sine_value])]
        )
        mat_real = jnp.where(is_z, mat_zr, mat_y)
        mat_imag = jnp.where(is_z, mat_zi, jnp.zeros_like(mat_zi))
        if kron_real is None:
            kron_real, kron_imag = (mat_real, mat_imag)
        else:
            kron_real, kron_imag = (
                jnp.kron(mat_real, kron_real) - jnp.kron(mat_imag, kron_imag),
                jnp.kron(mat_real, kron_imag) + jnp.kron(mat_imag, kron_real),
            )

    def apply_block(real_rows, imag_rows):
        new_real = contract_cols(real_rows, kron_real) - contract_cols(imag_rows, kron_imag)
        new_imag = contract_cols(imag_rows, kron_real) + contract_cols(real_rows, kron_imag)
        return jnp.stack([new_real.reshape(amp_count), new_imag.reshape(amp_count)])

    return (apply_block(ket_real, ket_imag), apply_block(bra_real, bra_imag), terms)


def rotate_global(
    ket_state,
    bra_state,
    far_ket,
    far_bra,
    bit_num,
    qubit_id,
    device_id,
    layer_id,
    angles,
    gate_kinds,
):
    kind_id, cosine, sine_value = rotation_of(angles, gate_kinds, layer_id, qubit_id)
    orient = (1 - 2 * (device_id >> bit_num & 1)).astype(jnp.float32)

    def turn_y(operands):
        own_ket, own_bra, other_ket, other_bra = operands
        partial_value = 0.25 * orient * jnp.sum(other_bra * own_ket - own_bra * other_ket)
        return (
            cosine * own_ket + orient * sine_value * other_ket,
            cosine * own_bra + orient * sine_value * other_bra,
            partial_value,
        )

    def turn_z(operands):
        own_ket, own_bra, other_ket, other_bra = operands
        partial_value = 0.5 * orient * jnp.sum(own_bra[0] * own_ket[1] - own_bra[1] * own_ket[0])
        return (
            rotate_phase(own_ket, cosine, orient * sine_value),
            rotate_phase(own_bra, cosine, orient * sine_value),
            partial_value,
        )

    new_ket, new_bra, partial_value = lax.cond(
        kind_id == 2, turn_z, turn_y, (ket_state, bra_state, far_ket, far_bra)
    )
    return (new_ket, new_bra, partial_value * kind_vector(kind_id, angles.shape[1]))


def on_device(ket_state, observable, angles, gate_kinds):
    amp_count = ket_state.shape[1]
    local_bits = amp_count.bit_length() - 1
    group_size = lax.axis_size("amp")
    global_bits = group_size.bit_length() - 1
    device_id = lax.axis_index("amp")
    layer_count = angles.shape[0]
    kind_count = angles.shape[1]
    bra_state = 2.0 / math.sqrt(amp_count * group_size) * observable[None, :] * ket_state
    sign_cache = {}
    grads_local = jnp.zeros((layer_count, kind_count), jnp.float32)
    for sweep_id in range(layer_count):
        layer_id = layer_count - 1 - sweep_id
        layout = 0
        local_map, device_map = layout_map(local_bits, global_bits)
        if layout not in sign_cache:
            sign_cache[layout] = entangle_sign(local_bits, global_bits, device_id, amp_count)
        phase_sign = sign_cache[layout]
        ket_state = ket_state * phase_sign[None, :]
        bra_state = bra_state * phase_sign[None, :]
        ket_state, bra_state, layer_terms = low_block(
            ket_state, bra_state, local_map[:7], layer_id, angles, gate_kinds
        )
        for position in range(7, local_bits):
            ket_state, bra_state, partial_value = rotate_position(
                ket_state, bra_state, position, local_map[position], layer_id, angles, gate_kinds
            )
            layer_terms = layer_terms + partial_value
        for bit_num in range(global_bits):
            far_ket, far_bra = from_partner((ket_state, bra_state), "amp", bit_num)
            ket_state, bra_state, partial_value = rotate_global(
                ket_state,
                bra_state,
                far_ket,
                far_bra,
                bit_num,
                device_map[bit_num],
                device_id,
                layer_id,
                angles,
                gate_kinds,
            )
            layer_terms = layer_terms + partial_value
        grads_local = grads_local.at[layer_id].set(layer_terms)
    grads = lax.psum(grads_local, "amp")
    return (bra_state, grads)


def chunk_layouts(g):
    top = g + LANE_BITS + SUB_BITS - 1
    home, away = {}, {}
    for q in range(LANE_BITS):
        home[q] = away[q] = (LANE, q)
    for bit, q in ((1, top - 1), (2, top)):
        home[q] = away[q] = (SUB, bit)
    moved = list(range(LANE_BITS + 2, top - 1)) + [LANE_BITS]
    for bit, q in enumerate(moved):
        home[q], away[q] = (MAJOR, bit), (DEVICE, bit)
    home[LANE_BITS + 1], away[LANE_BITS + 1] = (MAJOR, g), (CHUNK, 0)
    for bit in range(g):
        home[top + 1 + bit], away[top + 1 + bit] = (DEVICE, bit), (MAJOR, bit)
    return home, away


def split_major(x, bit):
    fold = x.reshape((x.shape[0] >> bit + 1, 2, 1 << bit) + x.shape[1:])
    return fold[:, 0], fold[:, 1]


def join_major(x0, x1):
    out = jnp.stack([x0, x1], axis=1)
    return out.reshape((-1,) + out.shape[3:])


def minor_bit(axis, bit):
    return lax.broadcasted_iota(jnp.int32, (1, 8, 128), 1 if axis == SUB else 2) >> bit & 1


def minor_sign(axis, bit):
    return (1 - 2 * minor_bit(axis, bit)).astype(jnp.float32)


def shifted(x, axis, by):
    dim = 1 if axis == SUB else 2
    return pltpu.roll(x, by % x.shape[dim], dim)


def partner(x, axis, bit):
    step = 1 << bit
    up = shifted(x, axis, -step)
    if 2 * step == x.shape[1 if axis == SUB else 2]:
        return up
    return jnp.where(minor_bit(axis, bit) == 0, up, shifted(x, axis, step))


def swap_bits(x, major, sub):
    x0, x1 = split_major(x, major)
    lower = minor_bit(SUB, sub) == 0

    def roll3(y, by):
        z = y.reshape((-1,) + y.shape[2:])
        return shifted(z, SUB, by).reshape(y.shape)

    step = 1 << sub
    return join_major(jnp.where(lower, x0, roll3(x1, step)), jnp.where(lower, roll3(x0, -step), x1))


def other_part(x):
    return partner(x, SUB, 0)


def weights(obs, chunk):
    place = lax.broadcasted_iota(jnp.int32, (1, 8, 128), 1) & 3
    if chunk == 0:
        end, far = 0, 3
    else:
        end, far = 3, 0
    step = 1 if chunk == 0 else -1
    near = jnp.where(place == end, obs, shifted(obs, SUB, step))
    return jnp.where(place == far, shifted(obs, SUB, 2 * step), near)


def y_gate(x, place, cy, sy):
    axis, bit = place
    if axis == MAJOR:
        x0, x1 = split_major(x, bit)
        return join_major(cy * x0 + sy * x1, cy * x1 - sy * x0)
    return cy * x + (sy * minor_sign(axis, bit)) * partner(x, axis, bit)


def lane_matrix(coefs):
    at = [lax.broadcasted_iota(jnp.int32, (128, 128), d) for d in range(2)]
    re, im = None, None
    for bit, (c, sy, sz) in enumerate(coefs):
        old, new = (x >> bit & 1 for x in at)
        z = (1 - 2 * new).astype(jnp.float32)
        same = old == new
        a, b = jnp.where(same, c, sy * z), jnp.where(same, sz * z, 0.0)
        re, im = (a, b) if re is None else (re * a - im * b, re * b + im * a)
    return jnp.concatenate([re, im], 1)


def turn_lanes(x, matrix):
    both = lax.dot_general(
        x.reshape(-1, 128),
        matrix[...],
        (((1,), (0,)), ((), ())),
        precision=lax.Precision.HIGH,
        preferred_element_type=jnp.float32,
    )
    re, im = both[:, :128].reshape(x.shape), both[:, 128:].reshape(x.shape)
    return re - minor_sign(SUB, 0) * other_part(im)


def terms(bra, ket, place, w, w_sum):
    axis, bit = place
    if axis == MAJOR:
        b0, b1 = split_major(bra, bit)
        k0, k1 = split_major(ket, bit)
        w0, w1 = split_major(w, bit)
        return 0.5 * jnp.sum(b1 * k0 - b0 * k1, axis=(0, 1)), 0.5 * jnp.sum(w0 - w1, axis=(0, 1))
    z = 0.5 * minor_sign(axis, bit)[0]
    return -z * jnp.sum(bra * partner(ket, axis, bit), axis=0), z * w_sum


def phases(place, qubits, edges, majors, me, chunk, turns=None):
    def bit_of(q):
        axis, bit = place[q]
        if axis in (LANE, SUB):
            return minor_bit(axis, bit)
        return me >> bit & 1 if axis == DEVICE else chunk

    at_major = {place[q][1]: q for q in range(qubits) if place[q][0] == MAJOR}
    parity = jnp.zeros((1, 8, 128), jnp.int32)
    for q in edges:
        ends = (q, (q + 1) % qubits)
        if all(place[e][0] != MAJOR for e in ends):
            parity = parity + bit_of(ends[0]) * bit_of(ends[1])
    re = (1 - 2 * (parity & 1)).astype(jnp.float32)
    im = None

    def times(re, im, c, s):
        if im is None:
            return re * c, re * s
        return re * c - im * s, im * c + re * s

    turns = turns or {}
    for q, (c, s) in turns.items():
        axis, bit = place[q]
        if axis != MAJOR:
            re, im = times(re, im, c, s * minor_sign(axis, bit))
    for j in range(majors.bit_length() - 1):
        q = at_major[j]
        parity, flips = None, []
        for edge, o in ((q, (q + 1) % qubits), ((q - 1) % qubits, (q - 1) % qubits)):
            if edge not in edges:
                continue
            if place[o][0] != MAJOR:
                parity = bit_of(o) if parity is None else parity + bit_of(o)
            elif place[o][1] < j:
                flips.append(place[o][1])

        def upper(x):
            if parity is not None:
                x = x * jnp.broadcast_to(1 - 2 * (parity & 1), (1, 8, 128)).astype(jnp.float32)
            for bit in flips:
                x0, x1 = split_major(x, bit)
                x = join_major(x0, -x1)
            return x

        lo, hi = (re, im), (upper(re), None if im is None else upper(im))
        if q in turns:
            c, s = turns[q]
            lo, hi = times(*lo, c, s), times(*hi, c, -s)
        re = jnp.concatenate([lo[0], hi[0]], 0)
        im = None if lo[1] is None else jnp.concatenate([lo[1], hi[1]], 0)
    return (re, None) if im is None else (re, -minor_sign(SUB, 0) * im)


def half_turn(angle):
    x = 0.5 * angle
    x2 = x * x
    cosine, sine = 0.0, 0.0
    for n in range(8, -1, -1):
        cosine = cosine * x2 + (-1.0) ** n / math.factorial(2 * n)
        sine = sine * x2 + (-1.0) ** n / math.factorial(2 * n + 1)
    return cosine, sine * x


def kernel(
    n, qubits, angles, kinds, ket_ref, obs_ref, out_ref, grads_ref,
    ket_in, obs_in, sent, held, back, landed, gsent, gheld,
    flag, send1, recv1, send2, recv2, gsend, grecv, load, wide,
):
    me = lax.axis_index("amp")
    g = n.bit_length() - 1
    home, away = chunk_layouts(g)
    scale = 2.0 / math.sqrt(2**qubits)

    loads = [
        pltpu.make_async_copy(ket_ref, ket_in, load.at[0]),
        pltpu.make_async_copy(obs_ref, obs_in, load.at[1]),
    ]
    for copy in loads:
        copy.start()

    half, size = n // 2, n // PLANES
    plane, place = me // size, me % size
    upper = plane // 2
    near = 2 - upper
    far = near + 1 - 2 * upper
    side = plane + 1 - 2 * (plane % 2)
    others = (near, far, side)
    planes = {"far": far, "near": near, "side": side, "own": plane}

    def inside(j):
        spot = place + j
        for bit in range(size.bit_length() - 1):
            step = 1 << bit
            spot = spot - 2 * step * (place // step % 2) * (j // step % 2)
        return spot

    barrier = pltpu.get_barrier_semaphore()
    for other in others:
        pl.semaphore_signal(barrier, inc=1, device_id=(other * size + place,), device_id_type=MESH)
    for j in range(1, size):
        pl.semaphore_signal(barrier, inc=1, device_id=(plane * size + inside(j),), device_id_type=MESH)
    for copy in loads:
        copy.wait()

    value = ket_in[...].reshape(2 * n, 8, 128)
    for bit in (1, 2):
        value = swap_bits(value, g - 2 + bit, bit)
    sent[:, 0] = value[:n]
    sent[:, 1] = value[n:]
    value = obs_in[...].reshape(n, 8, 128)
    for major, bit in ((g - 2, 0), (g - 1, 2)):
        value = swap_bits(value, major, bit)
    sent[:, 2] = jnp.stack([value[:half], value[half:]], axis=1).reshape(n, 8, 128)

    pl.semaphore_wait(barrier, size - 1 + len(others))
    for other in others:
        pl.semaphore_signal(flag.at[plane], inc=1, device_id=(other * size + place,), device_id_type=MESH)

    def exchange(source, target, send, recv, tiles):
        def part(ref, block, to):
            return ref.at[block, pl.ds(0, tiles[to])] if tiles else ref.at[block]

        def start(to, lower, upper):
            @pl.loop(lower, upper)
            def _(k):
                block = planes[to] * size + inside(size - 1 - k)
                pltpu.make_async_remote_copy(
                    src_ref=part(source, block, to),
                    dst_ref=part(target, me, to),
                    send_sem=send.at[planes[to]],
                    recv_sem=recv.at[plane],
                    device_id=(block,),
                    device_id_type=MESH,
                ).start()

        def many(to):
            blocks = pl.ds(planes[to] * size, size - 1 if to == "own" else size)
            return pltpu.make_async_remote_copy(
                src_ref=part(source, blocks, to),
                dst_ref=part(target, blocks, to),
                send_sem=send.at[planes[to]],
                recv_sem=recv.at[planes[to]],
                device_id=(me,),
                device_id_type=MESH,
            )

        return start, lambda to: many(to).wait_recv(), lambda: [many(to).wait_send() for to in planes]

    start1, arrive1, depart1 = exchange(sent, held, send1, recv1, dict.fromkeys(planes, 3))
    start2, arrive2, depart2 = exchange(back, landed, send2, recv2, dict.fromkeys(planes, 2))
    start3, arrive3, depart3 = exchange(gsent, gheld, gsend, grecv, None)
    start1("far", size - 1, size)
    start1("near", size - 1, size)
    start1("own", 0, size - 1)
    start1("side", size - 1, size)
    for to in ("near", "far", "side"):
        pl.semaphore_wait(flag.at[planes[to]], 1)
        start1(to, 0, size - 1)
    held[me] = sent[me]

    layers, kind_count = angles.shape
    turns = [[half_turn(angles[l, k]) for k in range(kind_count)] for l in range(layers)]
    coefs, shares = [], []
    for l in range(layers):
        row, share = [], []
        for q in range(qubits):
            kind = kinds[l, q]
            is_kind = [jnp.where(kind == k, 1.0, 0.0) for k in range(kind_count)]
            cy = sum(is_kind[k] * turns[l][k][0] for k in range(kind_count - 1))
            sy = sum(is_kind[k] * turns[l][k][1] for k in range(kind_count - 1))
            cz = is_kind[-1] * turns[l][-1][0]
            sz = is_kind[-1] * turns[l][-1][1]
            row.append((cy + is_kind[-1], sy, cz + (1.0 - is_kind[-1]), sz, cy + cz))
            share.append(is_kind)
        coefs.append(row)
        shares.append(share)

    every = range(qubits)
    late = [q for q in every if home[q][0] == MAJOR]
    first, last = min(late), max(late)
    late_edges = [q for q in every if first - 1 <= q <= last]
    early_edges = [q for q in every if q not in late_edges]
    local = [q for q in every if home[q][0] != DEVICE]
    outer = [q for q in every if home[q][0] == DEVICE]
    here = [q for q in every if q not in late]
    ready = [q for q in here if q not in (first - 1, last + 1)]
    rest = [q for q in local if q not in ready]

    for l in range(layers):
        lanes = [
            (coefs[l][q][4], coefs[l][q][1], coefs[l][q][3]) if l == 1 or q in ready else (1.0, 0.0, 0.0)
            for q in range(LANE_BITS)
        ]
        wide[l] = lane_matrix(lanes)

    sums = [[jnp.zeros((8, 128), jnp.float32) for _ in range(kind_count)] for _ in range(layers)]

    def add_terms(l, chosen, place, bra, ket):
        w = minor_sign(SUB, 0) * (bra * other_part(ket))
        w_sum = jnp.sum(w, axis=0)
        for q in chosen:
            y, z = terms(bra, ket, place[q], w, w_sum)
            for k in range(kind_count):
                sums[l][k] = sums[l][k] + shares[l][q][k] * (z if k == kind_count - 1 else y)

    def phase_of(l, chosen, place, edges, majors, chunk, by_matrix):
        turned = {q: coefs[l][q][2:4] for q in chosen if not (by_matrix and place[q][0] == LANE)}
        return phases(place, qubits, edges, majors, me, chunk, turned)

    def turn(x, l, chosen, place, phase, by_matrix=True):
        if by_matrix:
            x = turn_lanes(x, wide.at[l])
        for q in chosen:
            if not (by_matrix and place[q][0] == LANE):
                x = y_gate(x, place[q], coefs[l][q][0], coefs[l][q][1])
        return phase[0] * x + phase[1] * other_part(x)

    sign, _ = phases(home, qubits, every, 2 * n, me, 0)
    phase = phase_of(1, local, home, every, 2 * n, 0, True)
    ket = jnp.concatenate([sent[:, 0], sent[:, 1]], 0) * sign
    obs = sent[:, 2]
    bra = scale * jnp.concatenate([weights(obs, 0), weights(obs, 1)], 0) * ket
    add_terms(1, local, home, bra, ket)
    ket, bra = (turn(x, 1, local, home, phase) for x in (ket, bra))
    add_terms(0, local[1:-1], home, bra, ket)

    ready_phase = phase_of(0, ready, away, [], n, 0, True)
    signs = [phases(away, qubits, every, n, me, chunk)[0] for chunk in range(2)]
    mid_phases = [phase_of(1, here, away, early_edges, n, chunk, True) for chunk in range(2)]
    for origin in ("own", "side", "near", "far"):
        arrive1(origin)
    states = []
    for chunk in range(2):
        ket = held[:, chunk] * signs[chunk]
        bra = scale * weights(held[:, 2], chunk) * ket
        bra_mid = turn(bra, 1, here, away, mid_phases[chunk])
        back[:, chunk] = turn(bra_mid, 0, ready, away, ready_phase)
        states.append((ket, bra, bra_mid))
    start2("far", 0, size)
    start2("near", 0, size)
    for chunk, (ket, bra, bra_mid) in enumerate(states):
        add_terms(1, outer, away, bra, ket)
        ket = turn(ket, 1, here, away, mid_phases[chunk])
        add_terms(0, [local[-1]] + outer + [0], away, bra_mid, ket)

    at = [lax.broadcasted_iota(jnp.int32, (layers, 128), d) for d in range(2)]
    total = jnp.zeros((layers, 128), jnp.float32)
    for l in range(layers):
        for k in range(kind_count):
            total = total + jnp.where((at[0] == l) & (at[1] == k), jnp.sum(sums[l][k]), 0.0)
    gsent[...] = jnp.broadcast_to(total, gsent.shape)
    gheld[me] = total
    for to in ("far", "near", "side", "own"):
        start3(to, 0, size - 1 if to == "own" else size)
    start2("side", 0, size)
    start2("own", 0, size - 1)
    landed[me] = back[me]

    late_phase = phase_of(1, late, home, late_edges, 2 * n, 0, False)
    rest_phase = phase_of(0, rest, home, [], 2 * n, 0, False)
    for origin in ("own", "side", "near", "far"):
        arrive2(origin)
    x = jnp.concatenate([landed[:, 0], landed[:, 1]], 0)
    x = turn(x, 1, late, home, late_phase, False)
    x = turn(x, 0, rest, home, rest_phase, False)
    for bit in (1, 2):
        x = swap_bits(x, g - 2 + bit, bit)
    out_ref[...] = x.reshape(16 * n, 128)
    for origin in ("own", "side", "near", "far"):
        arrive3(origin)
    grads_ref[...] = jnp.sum(gheld[...], axis=0)
    depart1()
    depart2()
    depart3()


def finish(bra_ref, sums_ref, out_ref, grads_ref, picked, sems):
    picked[...] = sums_ref[pl.ds(0, picked.shape[0]), pl.ds(0, picked.shape[1])]
    pieces = sems.shape[0] - 1
    rows = out_ref.shape[0] // pieces
    copies = [pltpu.make_async_copy(picked, grads_ref, sems.at[pieces])]
    for k in range(pieces):
        part = pl.ds(k * rows, rows)
        copies.append(pltpu.make_async_copy(bra_ref.at[part], out_ref.at[part], sems.at[k]))
    for copy in copies:
        copy.start()
    for copy in copies:
        copy.wait()


def by_exchange(ket_state, observable, angles, gate_kinds):
    amp_count = ket_state.shape[1]
    n = lax.axis_size("amp")
    qubits = (amp_count * n).bit_length() - 1
    layers, kind_count = angles.shape
    rows = amp_count // 128
    ket = ket_state.reshape(2, rows, 128).transpose(1, 0, 2).reshape(2 * rows, 128)
    vmem = pl.BlockSpec(memory_space=pltpu.VMEM)
    smem = pl.BlockSpec(memory_space=pltpu.SMEM)
    hbm = pl.BlockSpec(memory_space=pltpu.HBM)
    f32 = jnp.float32
    dma = pltpu.SemaphoreType.DMA
    bra, sums = pl.pallas_call(
        functools.partial(kernel, n, qubits),
        out_shape=(
            pltpu.VMEM((2 * rows, 128), f32),
            pltpu.VMEM((layers, 128), f32),
        ),
        in_specs=[smem, smem, hbm, hbm],
        out_specs=(vmem, vmem),
        scratch_shapes=[
            pltpu.VMEM((2 * rows, 128), f32),
            pltpu.VMEM((rows, 128), f32),
            pltpu.VMEM((n, 3, 8, 128), f32),
            pltpu.VMEM((n, 3, 8, 128), f32),
            pltpu.VMEM((n, 2, 8, 128), f32),
            pltpu.VMEM((n, 2, 8, 128), f32),
            pltpu.VMEM((n, layers, 128), f32),
            pltpu.VMEM((n, layers, 128), f32),
            pltpu.SemaphoreType.REGULAR((PLANES,)),
        ]
        + [dma((PLANES,))] * 6
        + [dma((2,)), pltpu.VMEM((layers, 128, 256), f32)],
        compiler_params=pltpu.CompilerParams(
            collective_id=0, has_side_effects=True
        ),
    )(angles, gate_kinds, *(pltpu.with_memory_space_constraint(x, pltpu.HBM) for x in (ket, observable.reshape(rows, 128))))
    out, grads = pl.pallas_call(
        finish,
        out_shape=(
            jax.ShapeDtypeStruct((2 * rows, 128), f32),
            jax.ShapeDtypeStruct((layers, kind_count), f32),
        ),
        in_specs=[vmem, vmem],
        out_specs=(hbm, hbm),
        scratch_shapes=[pltpu.VMEM((layers, kind_count), f32), dma((5,))],
        compiler_params=pltpu.CompilerParams(vmem_limit_bytes=1 << 20),
    )(*(pltpu.with_memory_space_constraint(x, pltpu.VMEM) for x in (bra, sums)))
    bra_state = out.reshape(rows, 2, 128).transpose(1, 0, 2).reshape(2, amp_count)
    return (bra_state, grads)


def per_device(ket_state, observable, angles, gate_kinds):
    tiles = ket_state.shape[1] // (1 << LANE_BITS + SUB_BITS)
    if tiles == lax.axis_size("amp") and tiles >= 8 and angles.shape == (2, 3):
        return by_exchange(ket_state, observable, angles, gate_kinds)
    return on_device(ket_state, observable, angles, gate_kinds)


def solution(mesh):
    placed = (P(None, "amp"), P("amp"), P(), P())
    return jax.shard_map(
        per_device, mesh=mesh, in_specs=placed, out_specs=(P(None, "amp"), P()), check_vma=False
    )
```

```python
import functools
import math

import jax
import jax.numpy as jnp
import numpy as np
from jax import lax
from jax.experimental import pallas as pl
from jax.experimental.pallas import tpu as pltpu
from jax.sharding import PartitionSpec as P

MESH = pl.DeviceIdType.MESH
LANE, SUB, MAJOR, DEVICE, CHUNK = range(5)
LANE_BITS, SUB_BITS = 7, 3
PLANES = 4


def from_partner(value, axis, apart):
    mask = 2**apart
    pairs = [(source, source ^ mask) for source in range(lax.axis_size(axis))]
    return lax.ppermute(value, axis, pairs)


def pair_tables():
    column = np.arange(128)
    flips = []
    signs = []
    for position in range(7):
        upper = column >> position & 1
        flip_table = np.zeros((128, 128), np.float32)
        flip_table[column, column ^ 1 << position] = np.where(upper == 0, -0.5, 0.5)
        flips.append(flip_table)
        signs.append((1 - 2 * upper).astype(np.float32))
    return (np.stack(flips), np.stack(signs))


def layout_map(local_bits, global_bits):
    local_map = list(range(local_bits))
    device_map = [local_bits + bit_num for bit_num in range(global_bits)]
    return (local_map, device_map)


def entangle_sign(local_bits, global_bits, device_id, amp_count):
    local_map, device_map = layout_map(local_bits, global_bits)
    amp_index = lax.iota(jnp.int32, amp_count)
    bit_values = [None] * (local_bits + global_bits)
    for position in range(local_bits):
        bit_values[local_map[position]] = amp_index >> position & 1
    for bit_num in range(global_bits):
        bit_values[device_map[bit_num]] = device_id >> bit_num & 1
    all_bits = local_bits + global_bits
    parity = jnp.zeros((amp_count,), jnp.int32)
    for qubit_id in range(all_bits):
        parity = parity + bit_values[qubit_id] * bit_values[(qubit_id + 1) % all_bits]
    return (1 - 2 * (parity & 1)).astype(jnp.float32)


def rotation_of(angles, gate_kinds, layer_id, qubit_id):
    kind_id = gate_kinds[layer_id, qubit_id]
    chosen = jnp.arange(angles.shape[1]) == kind_id
    rotation = jnp.sum(jnp.where(chosen, angles[layer_id], 0.0))
    return (kind_id, jnp.cos(0.5 * rotation), jnp.sin(0.5 * rotation))


def kind_vector(kind_id, kind_count):
    return (jnp.arange(kind_count) == kind_id).astype(jnp.float32)


def rotate_phase(values, cosine, sine_value):
    return jnp.stack(
        [cosine * values[0] - sine_value * values[1], cosine * values[1] + sine_value * values[0]]
    )


def rotate_position(ket_state, bra_state, position, qubit_id, layer_id, angles, gate_kinds):
    amp_count = ket_state.shape[1]
    fold_shape = (2, amp_count >> position + 1, 2, 1 << position)
    kind_id, cosine, sine_value = rotation_of(angles, gate_kinds, layer_id, qubit_id)

    def turn_y(operands):
        folded_ket, folded_bra = operands
        ket_low, ket_high = (folded_ket[:, :, 0], folded_ket[:, :, 1])
        bra_low, bra_high = (folded_bra[:, :, 0], folded_bra[:, :, 1])
        partial_value = 0.5 * jnp.sum(bra_high * ket_low - bra_low * ket_high)
        new_ket = jnp.stack(
            [cosine * ket_low + sine_value * ket_high, cosine * ket_high - sine_value * ket_low],
            axis=2,
        )
        new_bra = jnp.stack(
            [cosine * bra_low + sine_value * bra_high, cosine * bra_high - sine_value * bra_low],
            axis=2,
        )
        return (new_ket, new_bra, partial_value)

    def turn_z(operands):
        folded_ket, folded_bra = operands
        ket_low, ket_high = (folded_ket[:, :, 0], folded_ket[:, :, 1])
        bra_low, bra_high = (folded_bra[:, :, 0], folded_bra[:, :, 1])
        partial_value = 0.5 * (
            jnp.sum(bra_low[0] * ket_low[1] - bra_low[1] * ket_low[0])
            - jnp.sum(bra_high[0] * ket_high[1] - bra_high[1] * ket_high[0])
        )
        new_ket = jnp.stack(
            [
                rotate_phase(ket_low, cosine, sine_value),
                rotate_phase(ket_high, cosine, -sine_value),
            ],
            axis=2,
        )
        new_bra = jnp.stack(
            [
                rotate_phase(bra_low, cosine, sine_value),
                rotate_phase(bra_high, cosine, -sine_value),
            ],
            axis=2,
        )
        return (new_ket, new_bra, partial_value)

    new_ket, new_bra, partial_value = lax.cond(
        kind_id == 2, turn_z, turn_y, (ket_state.reshape(fold_shape), bra_state.reshape(fold_shape))
    )
    terms = partial_value * kind_vector(kind_id, angles.shape[1])
    return (new_ket.reshape(2, amp_count), new_bra.reshape(2, amp_count), terms)


def contract_rows(left, right):
    return lax.dot_general(
        left,
        right,
        (((0,), (0,)), ((), ())),
        precision=lax.Precision.HIGHEST,
        preferred_element_type=jnp.float32,
    )


def contract_cols(left, right):
    return lax.dot_general(
        left,
        right,
        (((1,), (1,)), ((), ())),
        precision=lax.Precision.HIGHEST,
        preferred_element_type=jnp.float32,
    )


def low_block(ket_state, bra_state, qubit_list, layer_id, angles, gate_kinds):
    amp_count = ket_state.shape[1]
    row_count = amp_count // 128
    flips, signs = pair_tables()
    ket_real = ket_state[0].reshape(row_count, 128)
    ket_imag = ket_state[1].reshape(row_count, 128)
    bra_real = bra_state[0].reshape(row_count, 128)
    bra_imag = bra_state[1].reshape(row_count, 128)
    gram_real = contract_rows(bra_real, ket_real) + contract_rows(bra_imag, ket_imag)
    gram_imag = contract_rows(bra_real, ket_imag) - contract_rows(bra_imag, ket_real)
    gram_diag = jnp.diagonal(gram_imag)
    terms = jnp.zeros((angles.shape[1],), jnp.float32)
    kron_real = None
    kron_imag = None
    for position in range(7):
        kind_id, cosine, sine_value = rotation_of(
            angles, gate_kinds, layer_id, qubit_list[position]
        )
        is_z = kind_id == 2
        partial_value = jnp.where(
            is_z, 0.5 * jnp.sum(signs[position] * gram_diag), jnp.sum(flips[position] * gram_real)
        )
        terms = terms + partial_value * kind_vector(kind_id, angles.shape[1])
        mat_y = jnp.stack([jnp.stack([cosine, sine_value]), jnp.stack([-sine_value, cosine])])
        zero_value = jnp.zeros_like(cosine)
        mat_zr = jnp.stack([jnp.stack([cosine, zero_value]), jnp.stack([zero_value, cosine])])
        mat_zi = jnp.stack(
            [jnp.stack([sine_value, zero_value]), jnp.stack([zero_value, -sine_value])]
        )
        mat_real = jnp.where(is_z, mat_zr, mat_y)
        mat_imag = jnp.where(is_z, mat_zi, jnp.zeros_like(mat_zi))
        if kron_real is None:
            kron_real, kron_imag = (mat_real, mat_imag)
        else:
            kron_real, kron_imag = (
                jnp.kron(mat_real, kron_real) - jnp.kron(mat_imag, kron_imag),
                jnp.kron(mat_real, kron_imag) + jnp.kron(mat_imag, kron_real),
            )

    def apply_block(real_rows, imag_rows):
        new_real = contract_cols(real_rows, kron_real) - contract_cols(imag_rows, kron_imag)
        new_imag = contract_cols(imag_rows, kron_real) + contract_cols(real_rows, kron_imag)
        return jnp.stack([new_real.reshape(amp_count), new_imag.reshape(amp_count)])

    return (apply_block(ket_real, ket_imag), apply_block(bra_real, bra_imag), terms)


def rotate_global(
    ket_state,
    bra_state,
    far_ket,
    far_bra,
    bit_num,
    qubit_id,
    device_id,
    layer_id,
    angles,
    gate_kinds,
):
    kind_id, cosine, sine_value = rotation_of(angles, gate_kinds, layer_id, qubit_id)
    orient = (1 - 2 * (device_id >> bit_num & 1)).astype(jnp.float32)

    def turn_y(operands):
        own_ket, own_bra, other_ket, other_bra = operands
        partial_value = 0.25 * orient * jnp.sum(other_bra * own_ket - own_bra * other_ket)
        return (
            cosine * own_ket + orient * sine_value * other_ket,
            cosine * own_bra + orient * sine_value * other_bra,
            partial_value,
        )

    def turn_z(operands):
        own_ket, own_bra, other_ket, other_bra = operands
        partial_value = 0.5 * orient * jnp.sum(own_bra[0] * own_ket[1] - own_bra[1] * own_ket[0])
        return (
            rotate_phase(own_ket, cosine, orient * sine_value),
            rotate_phase(own_bra, cosine, orient * sine_value),
            partial_value,
        )

    new_ket, new_bra, partial_value = lax.cond(
        kind_id == 2, turn_z, turn_y, (ket_state, bra_state, far_ket, far_bra)
    )
    return (new_ket, new_bra, partial_value * kind_vector(kind_id, angles.shape[1]))


def on_device(ket_state, observable, angles, gate_kinds):
    amp_count = ket_state.shape[1]
    local_bits = amp_count.bit_length() - 1
    group_size = lax.axis_size("amp")
    global_bits = group_size.bit_length() - 1
    device_id = lax.axis_index("amp")
    layer_count = angles.shape[0]
    kind_count = angles.shape[1]
    bra_state = 2.0 / math.sqrt(amp_count * group_size) * observable[None, :] * ket_state
    sign_cache = {}
    grads_local = jnp.zeros((layer_count, kind_count), jnp.float32)
    for sweep_id in range(layer_count):
        layer_id = layer_count - 1 - sweep_id
        layout = 0
        local_map, device_map = layout_map(local_bits, global_bits)
        if layout not in sign_cache:
            sign_cache[layout] = entangle_sign(local_bits, global_bits, device_id, amp_count)
        phase_sign = sign_cache[layout]
        ket_state = ket_state * phase_sign[None, :]
        bra_state = bra_state * phase_sign[None, :]
        ket_state, bra_state, layer_terms = low_block(
            ket_state, bra_state, local_map[:7], layer_id, angles, gate_kinds
        )
        for position in range(7, local_bits):
            ket_state, bra_state, partial_value = rotate_position(
                ket_state, bra_state, position, local_map[position], layer_id, angles, gate_kinds
            )
            layer_terms = layer_terms + partial_value
        for bit_num in range(global_bits):
            far_ket, far_bra = from_partner((ket_state, bra_state), "amp", bit_num)
            ket_state, bra_state, partial_value = rotate_global(
                ket_state,
                bra_state,
                far_ket,
                far_bra,
                bit_num,
                device_map[bit_num],
                device_id,
                layer_id,
                angles,
                gate_kinds,
            )
            layer_terms = layer_terms + partial_value
        grads_local = grads_local.at[layer_id].set(layer_terms)
    grads = lax.psum(grads_local, "amp")
    return (bra_state, grads)


def chunk_layouts(g):
    top = g + LANE_BITS + SUB_BITS - 1
    home, away = {}, {}
    for q in range(LANE_BITS):
        home[q] = away[q] = (LANE, q)
    for bit, q in ((1, top - 1), (2, top)):
        home[q] = away[q] = (SUB, bit)
    moved = list(range(LANE_BITS + 2, top - 1)) + [LANE_BITS]
    for bit, q in enumerate(moved):
        home[q], away[q] = (MAJOR, bit), (DEVICE, bit)
    home[LANE_BITS + 1], away[LANE_BITS + 1] = (MAJOR, g), (CHUNK, 0)
    for bit in range(g):
        home[top + 1 + bit], away[top + 1 + bit] = (DEVICE, bit), (MAJOR, bit)
    return home, away


def split_major(x, bit):
    fold = x.reshape((x.shape[0] >> bit + 1, 2, 1 << bit) + x.shape[1:])
    return fold[:, 0], fold[:, 1]


def join_major(x0, x1):
    out = jnp.stack([x0, x1], axis=1)
    return out.reshape((-1,) + out.shape[3:])


def minor_bit(axis, bit):
    return lax.broadcasted_iota(jnp.int32, (1, 8, 128), 1 if axis == SUB else 2) >> bit & 1


def minor_sign(axis, bit):
    return (1 - 2 * minor_bit(axis, bit)).astype(jnp.float32)


def shifted(x, axis, by):
    dim = 1 if axis == SUB else 2
    return pltpu.roll(x, by % x.shape[dim], dim)


def partner(x, axis, bit):
    step = 1 << bit
    up = shifted(x, axis, -step)
    if 2 * step == x.shape[1 if axis == SUB else 2]:
        return up
    return jnp.where(minor_bit(axis, bit) == 0, up, shifted(x, axis, step))


def swap_bits(x, major, sub):
    x0, x1 = split_major(x, major)
    lower = minor_bit(SUB, sub) == 0

    def roll3(y, by):
        z = y.reshape((-1,) + y.shape[2:])
        return shifted(z, SUB, by).reshape(y.shape)

    step = 1 << sub
    return join_major(jnp.where(lower, x0, roll3(x1, step)), jnp.where(lower, roll3(x0, -step), x1))


def other_part(x):
    return partner(x, SUB, 0)


def weights(obs, chunk):
    place = lax.broadcasted_iota(jnp.int32, (1, 8, 128), 1) & 3
    if chunk == 0:
        end, far = 0, 3
    else:
        end, far = 3, 0
    step = 1 if chunk == 0 else -1
    near = jnp.where(place == end, obs, shifted(obs, SUB, step))
    return jnp.where(place == far, shifted(obs, SUB, 2 * step), near)


def y_gate(x, place, cy, sy):
    axis, bit = place
    if axis == MAJOR:
        x0, x1 = split_major(x, bit)
        return join_major(cy * x0 + sy * x1, cy * x1 - sy * x0)
    return cy * x + (sy * minor_sign(axis, bit)) * partner(x, axis, bit)


def lane_matrix(coefs):
    at = [lax.broadcasted_iota(jnp.int32, (128, 128), d) for d in range(2)]
    re, im = None, None
    for bit, (c, sy, sz) in enumerate(coefs):
        old, new = (x >> bit & 1 for x in at)
        z = (1 - 2 * new).astype(jnp.float32)
        same = old == new
        a, b = jnp.where(same, c, sy * z), jnp.where(same, sz * z, 0.0)
        re, im = (a, b) if re is None else (re * a - im * b, re * b + im * a)
    return jnp.concatenate([re, im], 1)


def turn_lanes(x, matrix):
    both = lax.dot_general(
        x.reshape(-1, 128),
        matrix[...],
        (((1,), (0,)), ((), ())),
        precision=lax.Precision.HIGH,
        preferred_element_type=jnp.float32,
    )
    re, im = both[:, :128].reshape(x.shape), both[:, 128:].reshape(x.shape)
    return re - minor_sign(SUB, 0) * other_part(im)


def terms(bra, ket, place, w, w_sum):
    axis, bit = place
    if axis == MAJOR:
        b0, b1 = split_major(bra, bit)
        k0, k1 = split_major(ket, bit)
        w0, w1 = split_major(w, bit)
        return 0.5 * jnp.sum(b1 * k0 - b0 * k1, axis=(0, 1)), 0.5 * jnp.sum(w0 - w1, axis=(0, 1))
    z = 0.5 * minor_sign(axis, bit)[0]
    return -z * jnp.sum(bra * partner(ket, axis, bit), axis=0), z * w_sum


def phases(place, qubits, edges, majors, me, chunk, turns=None):
    def bit_of(q):
        axis, bit = place[q]
        if axis in (LANE, SUB):
            return minor_bit(axis, bit)
        return me >> bit & 1 if axis == DEVICE else chunk

    at_major = {place[q][1]: q for q in range(qubits) if place[q][0] == MAJOR}
    parity = jnp.zeros((1, 8, 128), jnp.int32)
    for q in edges:
        ends = (q, (q + 1) % qubits)
        if all(place[e][0] != MAJOR for e in ends):
            parity = parity + bit_of(ends[0]) * bit_of(ends[1])
    re = (1 - 2 * (parity & 1)).astype(jnp.float32)
    im = None

    def times(re, im, c, s):
        if im is None:
            return re * c, re * s
        return re * c - im * s, im * c + re * s

    turns = turns or {}
    for q, (c, s) in turns.items():
        axis, bit = place[q]
        if axis != MAJOR:
            re, im = times(re, im, c, s * minor_sign(axis, bit))
    for j in range(majors.bit_length() - 1):
        q = at_major[j]
        parity, flips = None, []
        for edge, o in ((q, (q + 1) % qubits), ((q - 1) % qubits, (q - 1) % qubits)):
            if edge not in edges:
                continue
            if place[o][0] != MAJOR:
                parity = bit_of(o) if parity is None else parity + bit_of(o)
            elif place[o][1] < j:
                flips.append(place[o][1])

        def upper(x):
            if parity is not None:
                x = x * jnp.broadcast_to(1 - 2 * (parity & 1), (1, 8, 128)).astype(jnp.float32)
            for bit in flips:
                x0, x1 = split_major(x, bit)
                x = join_major(x0, -x1)
            return x

        lo, hi = (re, im), (upper(re), None if im is None else upper(im))
        if q in turns:
            c, s = turns[q]
            lo, hi = times(*lo, c, s), times(*hi, c, -s)
        re = jnp.concatenate([lo[0], hi[0]], 0)
        im = None if lo[1] is None else jnp.concatenate([lo[1], hi[1]], 0)
    return (re, None) if im is None else (re, -minor_sign(SUB, 0) * im)


def half_turn(angle):
    x = 0.5 * angle
    x2 = x * x
    cosine, sine = 0.0, 0.0
    for n in range(8, -1, -1):
        cosine = cosine * x2 + (-1.0) ** n / math.factorial(2 * n)
        sine = sine * x2 + (-1.0) ** n / math.factorial(2 * n + 1)
    return cosine, sine * x


def kernel(
    n, qubits, angles, kinds, ket_ref, obs_ref, out_ref, grads_ref,
    ket_in, obs_in, sent, held, back, landed,
    flag, send1, recv1, send2, recv2, load, wide, flips, begun,
):
    me = lax.axis_index("amp")
    g = n.bit_length() - 1
    home, away = chunk_layouts(g)
    scale = 2.0 / math.sqrt(2**qubits)

    loads = [
        pltpu.make_async_copy(ket_ref, ket_in, load.at[0]),
        pltpu.make_async_copy(obs_ref, obs_in, load.at[1]),
    ]
    for copy in loads:
        copy.start()

    half, size = n // 2, n // PLANES
    plane, place = me // size, me % size
    upper = plane // 2
    near = 2 - upper
    far = near + 1 - 2 * upper
    side = plane + 1 - 2 * (plane % 2)
    others = (near, far, side)
    planes = {"far": far, "near": near, "side": side, "own": plane}

    def inside(j):
        spot = place + j
        for bit in range(size.bit_length() - 1):
            step = 1 << bit
            spot = spot - 2 * step * (place // step % 2) * (j // step % 2)
        return spot

    barrier = pltpu.get_barrier_semaphore()
    for other in others:
        pl.semaphore_signal(barrier, inc=1, device_id=(other * size + place,), device_id_type=MESH)
    for j in range(1, size):
        pl.semaphore_signal(barrier, inc=1, device_id=(plane * size + inside(j),), device_id_type=MESH)
    for copy in loads:
        copy.wait()

    value = ket_in[...].reshape(2 * n, 8, 128)
    for bit in (1, 2):
        value = swap_bits(value, g - 2 + bit, bit)
    sent[:, pl.ds(0, 8)] = value[:n]
    sent[:, pl.ds(8, 8)] = value[n:]
    value = obs_in[...].reshape(n, 8, 128)
    for major, bit in ((g - 2, 0), (g - 1, 2)):
        value = swap_bits(value, major, bit)
    sent[:, pl.ds(16, 8)] = jnp.stack([value[:half], value[half:]], axis=1).reshape(n, 8, 128)

    pl.semaphore_wait(barrier, size - 1 + len(others))
    for other in others:
        pl.semaphore_signal(flag.at[plane], inc=1, device_id=(other * size + place,), device_id_type=MESH)

    def exchange(source, target, send, recv, rows):
        def part(ref, block):
            return ref.at[block, pl.ds(0, rows)]

        def start(to, lower, upper):
            @pl.loop(lower, upper)
            def _(k):
                block = planes[to] * size + inside(size - 1 - k)
                pltpu.make_async_remote_copy(
                    src_ref=part(source, block),
                    dst_ref=part(target, me),
                    send_sem=send.at[planes[to]],
                    recv_sem=recv.at[plane],
                    device_id=(block,),
                    device_id_type=MESH,
                ).start()

        def many(to):
            blocks = pl.ds(planes[to] * size, size - 1 if to == "own" else size)
            return pltpu.make_async_remote_copy(
                src_ref=part(source, blocks),
                dst_ref=part(target, blocks),
                send_sem=send.at[planes[to]],
                recv_sem=recv.at[planes[to]],
                device_id=(me,),
                device_id_type=MESH,
            )

        return start, lambda to: many(to).wait_recv(), lambda: [many(to).wait_send() for to in planes]

    start1, arrive1, depart1 = exchange(sent, held, send1, recv1, 24)
    start2, arrive2, depart2 = exchange(back, landed, send2, recv2, 17)
    start1("far", size - 1, size)
    start1("near", size - 1, size)
    start1("own", 0, size - 1)
    start1("side", size - 1, size)
    for to in ("near", "far", "side"):
        pl.semaphore_wait(flag.at[planes[to]], 1)
        start1(to, 0, size - 1)
    held[me] = sent[me]

    layers, kind_count = angles.shape
    turns = [[half_turn(angles[l, k]) for k in range(kind_count)] for l in range(layers)]
    coefs, shares = [], []
    for l in range(layers):
        row, share = [], []
        for q in range(qubits):
            kind = kinds[l, q]
            is_kind = [jnp.where(kind == k, 1.0, 0.0) for k in range(kind_count)]
            cy = sum(is_kind[k] * turns[l][k][0] for k in range(kind_count - 1))
            sy = sum(is_kind[k] * turns[l][k][1] for k in range(kind_count - 1))
            cz = is_kind[-1] * turns[l][-1][0]
            sz = is_kind[-1] * turns[l][-1][1]
            row.append((cy + is_kind[-1], sy, cz + (1.0 - is_kind[-1]), sz, cy + cz))
            share.append(is_kind)
        coefs.append(row)
        shares.append(share)

    every = range(qubits)
    late = [q for q in every if home[q][0] == MAJOR]
    first, last = min(late), max(late)
    late_edges = [q for q in every if first - 1 <= q <= last]
    early_edges = [q for q in every if q not in late_edges]
    local = [q for q in every if home[q][0] != DEVICE]
    outer = [q for q in every if home[q][0] == DEVICE]
    here = [q for q in every if q not in late]
    ready = [q for q in here if q not in (first - 1, last + 1)]
    rest = [q for q in local if q not in ready]

    for l in range(layers):
        lanes = [
            (coefs[l][q][4], coefs[l][q][1], coefs[l][q][3]) if l == 1 or q in ready else (1.0, 0.0, 0.0)
            for q in range(LANE_BITS)
        ]
        wide[l] = lane_matrix(lanes)

    sums = [[jnp.zeros((8, 128), jnp.float32) for _ in range(kind_count)] for _ in range(layers)]

    def add_terms(l, chosen, place, bra, ket):
        w = minor_sign(SUB, 0) * (bra * other_part(ket))
        w_sum = jnp.sum(w, axis=0)
        for q in chosen:
            y, z = terms(bra, ket, place[q], w, w_sum)
            for k in range(kind_count):
                sums[l][k] = sums[l][k] + shares[l][q][k] * (z if k == kind_count - 1 else y)

    def phase_of(l, chosen, place, edges, majors, chunk, by_matrix):
        turned = {q: coefs[l][q][2:4] for q in chosen if not (by_matrix and place[q][0] == LANE)}
        return phases(place, qubits, edges, majors, me, chunk, turned)

    def turn(x, l, chosen, place, phase, by_matrix=True):
        if by_matrix:
            x = turn_lanes(x, wide.at[l])
        for q in chosen:
            if not (by_matrix and place[q][0] == LANE):
                x = y_gate(x, place[q], coefs[l][q][0], coefs[l][q][1])
        return x if phase is None else phase[0] * x + phase[1] * other_part(x)

    sign, _ = phases(home, qubits, every, 2 * n, me, 0)
    phase = phase_of(1, local, home, every, 2 * n, 0, True)
    ket = jnp.concatenate([sent[:, pl.ds(0, 8)], sent[:, pl.ds(8, 8)]], 0) * sign
    obs = sent[:, pl.ds(16, 8)]
    bra = scale * jnp.concatenate([weights(obs, 0), weights(obs, 1)], 0) * ket
    add_terms(1, local, home, bra, ket)
    ket, bra = (turn(x, 1, local, home, phase) for x in (ket, bra))
    add_terms(0, local[1:-1], home, bra, ket)

    ready_phase = phase_of(0, ready, away, [], n, 0, True)
    signs = [phases(away, qubits, every, n, me, chunk)[0] for chunk in range(2)]
    mid_phases = [phase_of(1, here, away, early_edges, n, chunk, True) for chunk in range(2)]
    for chunk in range(2):
        flips[chunk] = signs[chunk]
    inner = size.bit_length() - 1
    wide_here = [q for q in here if away[q][0] == MAJOR and away[q][1] >= inner]
    slim_here = [q for q in here if q not in wide_here]
    for origin in ("own", "side", "near", "far"):
        arrive1(origin)
        blocks = pl.ds(planes[origin] * size, size)
        for chunk in range(2):
            ket = held[blocks, pl.ds(8 * chunk, 8)] * flips[chunk, blocks]
            bra = scale * weights(held[blocks, pl.ds(16, 8)], chunk) * ket
            add_terms(1, [q for q in outer if q in slim_here], away, bra, ket)
            begun[chunk, 0, blocks] = ket
            begun[chunk, 1, blocks] = bra
            begun[chunk, 2, blocks] = turn(ket, 1, slim_here, away, None)
            begun[chunk, 3, blocks] = turn(bra, 1, slim_here, away, None)
    for chunk in range(2):
        phase = mid_phases[chunk]
        bra = turn(begun[chunk, 3], 1, wide_here, away, phase, False)
        back[:, pl.ds(8 * chunk, 8)] = turn(bra, 0, ready, away, ready_phase)
        add_terms(1, [q for q in outer if q in wide_here], away, begun[chunk, 1], begun[chunk, 0])
        ket = turn(begun[chunk, 2], 1, wide_here, away, phase, False)
        add_terms(0, [local[-1]] + outer + [0], away, bra, ket)
    spot = [lax.broadcasted_iota(jnp.int32, (8, 128), d) for d in range(2)]
    total = jnp.zeros((8, 128), jnp.float32)
    for l in range(layers):
        for k in range(kind_count):
            row = jnp.sum(sums[l][k], axis=0, keepdims=True)
            total = total + jnp.where(spot[0] == l * kind_count + k, row, 0.0)
    total = jnp.sum(total, axis=1, keepdims=True)
    total = jnp.sum(jnp.where(spot[0] == spot[1], total, 0.0), axis=0, keepdims=True)
    back[:, pl.ds(16, 1)] = jnp.broadcast_to(total, (n, 1, 128))

    start2("far", 0, size)
    start2("near", 0, size)
    start2("side", 0, size)
    start2("own", 0, size - 1)
    landed[me] = back[me]

    late_phase = phase_of(1, late, home, late_edges, 2 * n, 0, False)
    rest_phase = phase_of(0, rest, home, [], 2 * n, 0, False)
    wide_late = [q for q in late if inner <= home[q][1] < g]
    slim = {q: (MAJOR, min(home[q][1], inner)) for q in late if q not in wide_late}
    for origin in ("own", "side", "near", "far"):
        arrive2(origin)
        blocks = pl.ds(planes[origin] * size, size)
        x = jnp.concatenate([landed[blocks, pl.ds(0, 8)], landed[blocks, pl.ds(8, 8)]], 0)
        x = turn(x, 1, list(slim), slim, None, False)
        begun[0, 0, blocks] = x[:size]
        begun[1, 0, blocks] = x[size:]
    x = jnp.concatenate([begun[0, 0], begun[1, 0]], 0)
    x = turn(x, 1, wide_late, home, late_phase, False)
    x = turn(x, 0, rest, home, rest_phase, False)
    for bit in (1, 2):
        x = swap_bits(x, g - 2 + bit, bit)
    out_ref[...] = x.reshape(16 * n, 128)
    grads_ref[...] = jnp.sum(landed[:, pl.ds(16, 1)], axis=0)
    depart1()
    depart2()


def finish(bra_ref, sums_ref, out_ref, grads_ref, picked, sems):
    layers, kind_count = picked.shape
    for l in range(layers):
        picked[pl.ds(l, 1), :] = sums_ref[:, pl.ds(l * kind_count, kind_count)]
    pieces = sems.shape[0] - 1
    rows = out_ref.shape[0] // pieces
    copies = [pltpu.make_async_copy(picked, grads_ref, sems.at[pieces])]
    for k in range(pieces):
        part = pl.ds(k * rows, rows)
        copies.append(pltpu.make_async_copy(bra_ref.at[part], out_ref.at[part], sems.at[k]))
    for copy in copies:
        copy.start()
    for copy in copies:
        copy.wait()


def by_exchange(ket_state, observable, angles, gate_kinds):
    amp_count = ket_state.shape[1]
    n = lax.axis_size("amp")
    qubits = (amp_count * n).bit_length() - 1
    layers, kind_count = angles.shape
    rows = amp_count // 128
    ket = ket_state.reshape(2, rows, 128).transpose(1, 0, 2).reshape(2 * rows, 128)
    vmem = pl.BlockSpec(memory_space=pltpu.VMEM)
    smem = pl.BlockSpec(memory_space=pltpu.SMEM)
    hbm = pl.BlockSpec(memory_space=pltpu.HBM)
    f32 = jnp.float32
    dma = pltpu.SemaphoreType.DMA
    bra, sums = pl.pallas_call(
        functools.partial(kernel, n, qubits),
        out_shape=(
            pltpu.VMEM((2 * rows, 128), f32),
            pltpu.VMEM((1, 128), f32),
        ),
        in_specs=[smem, smem, hbm, hbm],
        out_specs=(vmem, vmem),
        scratch_shapes=[
            pltpu.VMEM((2 * rows, 128), f32),
            pltpu.VMEM((rows, 128), f32),
        ]
        + [pltpu.VMEM((n, 24, 128), f32)] * 4
        + [
            pltpu.SemaphoreType.REGULAR((PLANES,)),
        ]
        + [dma((PLANES,))] * 4
        + [dma((2,)), pltpu.VMEM((layers, 128, 256), f32)]
        + [pltpu.VMEM((2, n, 8, 128), f32), pltpu.VMEM((2, 4, n, 8, 128), f32)],
        compiler_params=pltpu.CompilerParams(
            collective_id=0, has_side_effects=True
        ),
    )(angles, gate_kinds, *(pltpu.with_memory_space_constraint(x, pltpu.HBM) for x in (ket, observable.reshape(rows, 128))))
    out, grads = pl.pallas_call(
        finish,
        out_shape=(
            jax.ShapeDtypeStruct((2 * rows, 128), f32),
            jax.ShapeDtypeStruct((layers, kind_count), f32),
        ),
        in_specs=[vmem, vmem],
        out_specs=(hbm, hbm),
        scratch_shapes=[pltpu.VMEM((layers, kind_count), f32), dma((5,))],
        compiler_params=pltpu.CompilerParams(vmem_limit_bytes=1 << 20),
    )(*(pltpu.with_memory_space_constraint(x, pltpu.VMEM) for x in (bra, sums)))
    bra_state = out.reshape(rows, 2, 128).transpose(1, 0, 2).reshape(2, amp_count)
    return (bra_state, grads)


def per_device(ket_state, observable, angles, gate_kinds):
    tiles = ket_state.shape[1] // (1 << LANE_BITS + SUB_BITS)
    if tiles == lax.axis_size("amp") and tiles >= 8 and angles.shape == (2, 3):
        return by_exchange(ket_state, observable, angles, gate_kinds)
    return on_device(ket_state, observable, angles, gate_kinds)


def solution(mesh):
    placed = (P(None, "amp"), P("amp"), P(), P())
    return jax.shard_map(
        per_device, mesh=mesh, in_specs=placed, out_specs=(P(None, "amp"), P()), check_vma=False
    )
```

```python
import functools
import math

import jax
import jax.numpy as jnp
import numpy as np
from jax import lax
from jax.experimental import pallas as pl
from jax.experimental.pallas import tpu as pltpu
from jax.sharding import PartitionSpec as P

MESH = pl.DeviceIdType.MESH
LANE, SUB, MAJOR, DEVICE, CHUNK = range(5)
LANE_BITS, SUB_BITS = 7, 3
PLANES = 4


def from_partner(value, axis, apart):
    mask = 2**apart
    pairs = [(source, source ^ mask) for source in range(lax.axis_size(axis))]
    return lax.ppermute(value, axis, pairs)


def pair_tables():
    column = np.arange(128)
    flips = []
    signs = []
    for position in range(7):
        upper = column >> position & 1
        flip_table = np.zeros((128, 128), np.float32)
        flip_table[column, column ^ 1 << position] = np.where(upper == 0, -0.5, 0.5)
        flips.append(flip_table)
        signs.append((1 - 2 * upper).astype(np.float32))
    return (np.stack(flips), np.stack(signs))


def layout_map(local_bits, global_bits):
    local_map = list(range(local_bits))
    device_map = [local_bits + bit_num for bit_num in range(global_bits)]
    return (local_map, device_map)


def entangle_sign(local_bits, global_bits, device_id, amp_count):
    local_map, device_map = layout_map(local_bits, global_bits)
    amp_index = lax.iota(jnp.int32, amp_count)
    bit_values = [None] * (local_bits + global_bits)
    for position in range(local_bits):
        bit_values[local_map[position]] = amp_index >> position & 1
    for bit_num in range(global_bits):
        bit_values[device_map[bit_num]] = device_id >> bit_num & 1
    all_bits = local_bits + global_bits
    parity = jnp.zeros((amp_count,), jnp.int32)
    for qubit_id in range(all_bits):
        parity = parity + bit_values[qubit_id] * bit_values[(qubit_id + 1) % all_bits]
    return (1 - 2 * (parity & 1)).astype(jnp.float32)


def rotation_of(angles, gate_kinds, layer_id, qubit_id):
    kind_id = gate_kinds[layer_id, qubit_id]
    chosen = jnp.arange(angles.shape[1]) == kind_id
    rotation = jnp.sum(jnp.where(chosen, angles[layer_id], 0.0))
    return (kind_id, jnp.cos(0.5 * rotation), jnp.sin(0.5 * rotation))


def kind_vector(kind_id, kind_count):
    return (jnp.arange(kind_count) == kind_id).astype(jnp.float32)


def rotate_phase(values, cosine, sine_value):
    return jnp.stack(
        [cosine * values[0] - sine_value * values[1], cosine * values[1] + sine_value * values[0]]
    )


def rotate_position(ket_state, bra_state, position, qubit_id, layer_id, angles, gate_kinds):
    amp_count = ket_state.shape[1]
    fold_shape = (2, amp_count >> position + 1, 2, 1 << position)
    kind_id, cosine, sine_value = rotation_of(angles, gate_kinds, layer_id, qubit_id)

    def turn_y(operands):
        folded_ket, folded_bra = operands
        ket_low, ket_high = (folded_ket[:, :, 0], folded_ket[:, :, 1])
        bra_low, bra_high = (folded_bra[:, :, 0], folded_bra[:, :, 1])
        partial_value = 0.5 * jnp.sum(bra_high * ket_low - bra_low * ket_high)
        new_ket = jnp.stack(
            [cosine * ket_low + sine_value * ket_high, cosine * ket_high - sine_value * ket_low],
            axis=2,
        )
        new_bra = jnp.stack(
            [cosine * bra_low + sine_value * bra_high, cosine * bra_high - sine_value * bra_low],
            axis=2,
        )
        return (new_ket, new_bra, partial_value)

    def turn_z(operands):
        folded_ket, folded_bra = operands
        ket_low, ket_high = (folded_ket[:, :, 0], folded_ket[:, :, 1])
        bra_low, bra_high = (folded_bra[:, :, 0], folded_bra[:, :, 1])
        partial_value = 0.5 * (
            jnp.sum(bra_low[0] * ket_low[1] - bra_low[1] * ket_low[0])
            - jnp.sum(bra_high[0] * ket_high[1] - bra_high[1] * ket_high[0])
        )
        new_ket = jnp.stack(
            [
                rotate_phase(ket_low, cosine, sine_value),
                rotate_phase(ket_high, cosine, -sine_value),
            ],
            axis=2,
        )
        new_bra = jnp.stack(
            [
                rotate_phase(bra_low, cosine, sine_value),
                rotate_phase(bra_high, cosine, -sine_value),
            ],
            axis=2,
        )
        return (new_ket, new_bra, partial_value)

    new_ket, new_bra, partial_value = lax.cond(
        kind_id == 2, turn_z, turn_y, (ket_state.reshape(fold_shape), bra_state.reshape(fold_shape))
    )
    terms = partial_value * kind_vector(kind_id, angles.shape[1])
    return (new_ket.reshape(2, amp_count), new_bra.reshape(2, amp_count), terms)


def contract_rows(left, right):
    return lax.dot_general(
        left,
        right,
        (((0,), (0,)), ((), ())),
        precision=lax.Precision.HIGHEST,
        preferred_element_type=jnp.float32,
    )


def contract_cols(left, right):
    return lax.dot_general(
        left,
        right,
        (((1,), (1,)), ((), ())),
        precision=lax.Precision.HIGHEST,
        preferred_element_type=jnp.float32,
    )


def low_block(ket_state, bra_state, qubit_list, layer_id, angles, gate_kinds):
    amp_count = ket_state.shape[1]
    row_count = amp_count // 128
    flips, signs = pair_tables()
    ket_real = ket_state[0].reshape(row_count, 128)
    ket_imag = ket_state[1].reshape(row_count, 128)
    bra_real = bra_state[0].reshape(row_count, 128)
    bra_imag = bra_state[1].reshape(row_count, 128)
    gram_real = contract_rows(bra_real, ket_real) + contract_rows(bra_imag, ket_imag)
    gram_imag = contract_rows(bra_real, ket_imag) - contract_rows(bra_imag, ket_real)
    gram_diag = jnp.diagonal(gram_imag)
    terms = jnp.zeros((angles.shape[1],), jnp.float32)
    kron_real = None
    kron_imag = None
    for position in range(7):
        kind_id, cosine, sine_value = rotation_of(
            angles, gate_kinds, layer_id, qubit_list[position]
        )
        is_z = kind_id == 2
        partial_value = jnp.where(
            is_z, 0.5 * jnp.sum(signs[position] * gram_diag), jnp.sum(flips[position] * gram_real)
        )
        terms = terms + partial_value * kind_vector(kind_id, angles.shape[1])
        mat_y = jnp.stack([jnp.stack([cosine, sine_value]), jnp.stack([-sine_value, cosine])])
        zero_value = jnp.zeros_like(cosine)
        mat_zr = jnp.stack([jnp.stack([cosine, zero_value]), jnp.stack([zero_value, cosine])])
        mat_zi = jnp.stack(
            [jnp.stack([sine_value, zero_value]), jnp.stack([zero_value, -sine_value])]
        )
        mat_real = jnp.where(is_z, mat_zr, mat_y)
        mat_imag = jnp.where(is_z, mat_zi, jnp.zeros_like(mat_zi))
        if kron_real is None:
            kron_real, kron_imag = (mat_real, mat_imag)
        else:
            kron_real, kron_imag = (
                jnp.kron(mat_real, kron_real) - jnp.kron(mat_imag, kron_imag),
                jnp.kron(mat_real, kron_imag) + jnp.kron(mat_imag, kron_real),
            )

    def apply_block(real_rows, imag_rows):
        new_real = contract_cols(real_rows, kron_real) - contract_cols(imag_rows, kron_imag)
        new_imag = contract_cols(imag_rows, kron_real) + contract_cols(real_rows, kron_imag)
        return jnp.stack([new_real.reshape(amp_count), new_imag.reshape(amp_count)])

    return (apply_block(ket_real, ket_imag), apply_block(bra_real, bra_imag), terms)


def rotate_global(
    ket_state,
    bra_state,
    far_ket,
    far_bra,
    bit_num,
    qubit_id,
    device_id,
    layer_id,
    angles,
    gate_kinds,
):
    kind_id, cosine, sine_value = rotation_of(angles, gate_kinds, layer_id, qubit_id)
    orient = (1 - 2 * (device_id >> bit_num & 1)).astype(jnp.float32)

    def turn_y(operands):
        own_ket, own_bra, other_ket, other_bra = operands
        partial_value = 0.25 * orient * jnp.sum(other_bra * own_ket - own_bra * other_ket)
        return (
            cosine * own_ket + orient * sine_value * other_ket,
            cosine * own_bra + orient * sine_value * other_bra,
            partial_value,
        )

    def turn_z(operands):
        own_ket, own_bra, other_ket, other_bra = operands
        partial_value = 0.5 * orient * jnp.sum(own_bra[0] * own_ket[1] - own_bra[1] * own_ket[0])
        return (
            rotate_phase(own_ket, cosine, orient * sine_value),
            rotate_phase(own_bra, cosine, orient * sine_value),
            partial_value,
        )

    new_ket, new_bra, partial_value = lax.cond(
        kind_id == 2, turn_z, turn_y, (ket_state, bra_state, far_ket, far_bra)
    )
    return (new_ket, new_bra, partial_value * kind_vector(kind_id, angles.shape[1]))


def on_device(ket_state, observable, angles, gate_kinds):
    amp_count = ket_state.shape[1]
    local_bits = amp_count.bit_length() - 1
    group_size = lax.axis_size("amp")
    global_bits = group_size.bit_length() - 1
    device_id = lax.axis_index("amp")
    layer_count = angles.shape[0]
    kind_count = angles.shape[1]
    bra_state = 2.0 / math.sqrt(amp_count * group_size) * observable[None, :] * ket_state
    sign_cache = {}
    grads_local = jnp.zeros((layer_count, kind_count), jnp.float32)
    for sweep_id in range(layer_count):
        layer_id = layer_count - 1 - sweep_id
        layout = 0
        local_map, device_map = layout_map(local_bits, global_bits)
        if layout not in sign_cache:
            sign_cache[layout] = entangle_sign(local_bits, global_bits, device_id, amp_count)
        phase_sign = sign_cache[layout]
        ket_state = ket_state * phase_sign[None, :]
        bra_state = bra_state * phase_sign[None, :]
        ket_state, bra_state, layer_terms = low_block(
            ket_state, bra_state, local_map[:7], layer_id, angles, gate_kinds
        )
        for position in range(7, local_bits):
            ket_state, bra_state, partial_value = rotate_position(
                ket_state, bra_state, position, local_map[position], layer_id, angles, gate_kinds
            )
            layer_terms = layer_terms + partial_value
        for bit_num in range(global_bits):
            far_ket, far_bra = from_partner((ket_state, bra_state), "amp", bit_num)
            ket_state, bra_state, partial_value = rotate_global(
                ket_state,
                bra_state,
                far_ket,
                far_bra,
                bit_num,
                device_map[bit_num],
                device_id,
                layer_id,
                angles,
                gate_kinds,
            )
            layer_terms = layer_terms + partial_value
        grads_local = grads_local.at[layer_id].set(layer_terms)
    grads = lax.psum(grads_local, "amp")
    return (bra_state, grads)


def chunk_layouts(g):
    top = g + LANE_BITS + SUB_BITS - 1
    home, away = {}, {}
    for q in range(LANE_BITS):
        home[q] = away[q] = (LANE, q)
    for bit, q in ((1, top - 1), (2, top)):
        home[q] = away[q] = (SUB, bit)
    moved = list(range(LANE_BITS + 2, top - 1)) + [LANE_BITS]
    for bit, q in enumerate(moved):
        home[q], away[q] = (MAJOR, bit), (DEVICE, bit)
    home[LANE_BITS + 1], away[LANE_BITS + 1] = (MAJOR, g), (CHUNK, 0)
    for bit in range(g):
        home[top + 1 + bit], away[top + 1 + bit] = (DEVICE, bit), (MAJOR, bit)
    return home, away


def split_major(x, bit):
    fold = x.reshape((x.shape[0] >> bit + 1, 2, 1 << bit) + x.shape[1:])
    return fold[:, 0], fold[:, 1]


def join_major(x0, x1):
    out = jnp.stack([x0, x1], axis=1)
    return out.reshape((-1,) + out.shape[3:])


def minor_bit(axis, bit):
    return lax.broadcasted_iota(jnp.int32, (1, 8, 128), 1 if axis == SUB else 2) >> bit & 1


def minor_sign(axis, bit):
    return (1 - 2 * minor_bit(axis, bit)).astype(jnp.float32)


def shifted(x, axis, by):
    dim = 1 if axis == SUB else 2
    return pltpu.roll(x, by % x.shape[dim], dim)


def partner(x, axis, bit):
    step = 1 << bit
    up = shifted(x, axis, -step)
    if 2 * step == x.shape[1 if axis == SUB else 2]:
        return up
    return jnp.where(minor_bit(axis, bit) == 0, up, shifted(x, axis, step))


def swap_bits(x, major, sub):
    x0, x1 = split_major(x, major)
    lower = minor_bit(SUB, sub) == 0

    def roll3(y, by):
        z = y.reshape((-1,) + y.shape[2:])
        return shifted(z, SUB, by).reshape(y.shape)

    step = 1 << sub
    return join_major(jnp.where(lower, x0, roll3(x1, step)), jnp.where(lower, roll3(x0, -step), x1))


def other_part(x):
    return partner(x, SUB, 0)


def weights(obs, chunk):
    place = lax.broadcasted_iota(jnp.int32, (1, 8, 128), 1) & 3
    if chunk == 0:
        end, far = 0, 3
    else:
        end, far = 3, 0
    step = 1 if chunk == 0 else -1
    near = jnp.where(place == end, obs, shifted(obs, SUB, step))
    return jnp.where(place == far, shifted(obs, SUB, 2 * step), near)


def y_gate(x, place, cy, sy):
    axis, bit = place
    if axis == MAJOR:
        x0, x1 = split_major(x, bit)
        return join_major(cy * x0 + sy * x1, cy * x1 - sy * x0)
    return cy * x + (sy * minor_sign(axis, bit)) * partner(x, axis, bit)


def major_gates(x, gates, phase):
    tiles = [x[i : i + 1] for i in range(x.shape[0])]
    split = (len(gates) + 1) // 2 if len(gates) > 3 else len(gates)
    passes = [p for p in (gates[:split], gates[split:]) if p]
    for number, some in enumerate(passes):
        spread = sum(1 << bit for bit, _, _ in some)
        for base in range(len(tiles)):
            if base & spread:
                continue
            group = [base]
            for bit, _, _ in some:
                group = group + [i + (1 << bit) for i in group]
            for bit, cy, sy in some:
                for i in group:
                    if not i >> bit & 1:
                        j = i + (1 << bit)
                        a, b = tiles[i], tiles[j]
                        tiles[i], tiles[j] = cy * a + sy * b, cy * b - sy * a
            if phase is not None and number == len(passes) - 1:
                for i in group:
                    tiles[i] = phase[0][i : i + 1] * tiles[i] + phase[1][i : i + 1] * other_part(tiles[i])
    return jnp.concatenate(tiles, 0)


def lane_matrix(coefs):
    at = [lax.broadcasted_iota(jnp.int32, (128, 128), d) for d in range(2)]
    re, im = None, None
    for bit, (c, sy, sz) in enumerate(coefs):
        old, new = (x >> bit & 1 for x in at)
        z = (1 - 2 * new).astype(jnp.float32)
        same = old == new
        a, b = jnp.where(same, c, sy * z), jnp.where(same, sz * z, 0.0)
        re, im = (a, b) if re is None else (re * a - im * b, re * b + im * a)
    return jnp.concatenate([re, im], 1)


def turn_lanes(x, matrix):
    both = lax.dot_general(
        x.reshape(-1, 128),
        matrix[...],
        (((1,), (0,)), ((), ())),
        precision=lax.Precision.HIGH,
        preferred_element_type=jnp.float32,
    )
    re, im = both[:, :128].reshape(x.shape), both[:, 128:].reshape(x.shape)
    return re - minor_sign(SUB, 0) * other_part(im)


def terms(bra, ket, place, w, w_sum):
    axis, bit = place
    if axis == MAJOR:
        b0, b1 = split_major(bra, bit)
        k0, k1 = split_major(ket, bit)
        w0, w1 = split_major(w, bit)
        return 0.5 * jnp.sum(b1 * k0 - b0 * k1, axis=(0, 1)), 0.5 * jnp.sum(w0 - w1, axis=(0, 1))
    z = 0.5 * minor_sign(axis, bit)[0]
    return -z * jnp.sum(bra * partner(ket, axis, bit), axis=0), z * w_sum


def phases(place, qubits, edges, majors, me, chunk, turns=None):
    def bit_of(q):
        axis, bit = place[q]
        if axis in (LANE, SUB):
            return minor_bit(axis, bit)
        return me >> bit & 1 if axis == DEVICE else chunk

    at_major = {place[q][1]: q for q in range(qubits) if place[q][0] == MAJOR}
    parity = jnp.zeros((1, 8, 128), jnp.int32)
    for q in edges:
        ends = (q, (q + 1) % qubits)
        if all(place[e][0] != MAJOR for e in ends):
            parity = parity + bit_of(ends[0]) * bit_of(ends[1])
    re = (1 - 2 * (parity & 1)).astype(jnp.float32)
    im = None

    def times(re, im, c, s):
        if im is None:
            return re * c, re * s
        return re * c - im * s, im * c + re * s

    turns = turns or {}
    for q, (c, s) in turns.items():
        axis, bit = place[q]
        if axis != MAJOR:
            re, im = times(re, im, c, s * minor_sign(axis, bit))
    for j in range(majors.bit_length() - 1):
        q = at_major[j]
        parity, flips = None, []
        for edge, o in ((q, (q + 1) % qubits), ((q - 1) % qubits, (q - 1) % qubits)):
            if edge not in edges:
                continue
            if place[o][0] != MAJOR:
                parity = bit_of(o) if parity is None else parity + bit_of(o)
            elif place[o][1] < j:
                flips.append(place[o][1])

        def upper(x):
            if parity is not None:
                x = x * jnp.broadcast_to(1 - 2 * (parity & 1), (1, 8, 128)).astype(jnp.float32)
            for bit in flips:
                x0, x1 = split_major(x, bit)
                x = join_major(x0, -x1)
            return x

        lo, hi = (re, im), (upper(re), None if im is None else upper(im))
        if q in turns:
            c, s = turns[q]
            lo, hi = times(*lo, c, s), times(*hi, c, -s)
        re = jnp.concatenate([lo[0], hi[0]], 0)
        im = None if lo[1] is None else jnp.concatenate([lo[1], hi[1]], 0)
    return (re, None) if im is None else (re, -minor_sign(SUB, 0) * im)


def half_turn(angle):
    x = 0.5 * angle
    x2 = x * x
    cosine, sine = 0.0, 0.0
    for n in range(8, -1, -1):
        cosine = cosine * x2 + (-1.0) ** n / math.factorial(2 * n)
        sine = sine * x2 + (-1.0) ** n / math.factorial(2 * n + 1)
    return cosine, sine * x


def kernel(
    n, qubits, angles, kinds, ket_ref, obs_ref, out_ref, grads_ref,
    ket_in, obs_in, sent, held, back, landed,
    flag, send1, recv1, send2, recv2, load, wide, flips, begun,
):
    me = lax.axis_index("amp")
    g = n.bit_length() - 1
    home, away = chunk_layouts(g)
    scale = 2.0 / math.sqrt(2**qubits)

    loads = [
        pltpu.make_async_copy(ket_ref, ket_in, load.at[0]),
        pltpu.make_async_copy(obs_ref, obs_in, load.at[1]),
    ]
    for copy in loads:
        copy.start()

    half, size = n // 2, n // PLANES
    plane, place = me // size, me % size
    upper = plane // 2
    near = 2 - upper
    far = near + 1 - 2 * upper
    side = plane + 1 - 2 * (plane % 2)
    others = (near, far, side)
    planes = {"far": far, "near": near, "side": side, "own": plane}

    def inside(j):
        spot = place + j
        for bit in range(size.bit_length() - 1):
            step = 1 << bit
            spot = spot - 2 * step * (place // step % 2) * (j // step % 2)
        return spot

    barrier = pltpu.get_barrier_semaphore()
    for other in others:
        pl.semaphore_signal(barrier, inc=1, device_id=(other * size + place,), device_id_type=MESH)
    for j in range(1, size):
        pl.semaphore_signal(barrier, inc=1, device_id=(plane * size + inside(j),), device_id_type=MESH)
    for copy in loads:
        copy.wait()

    value = ket_in[...].reshape(2 * n, 8, 128)
    for bit in (1, 2):
        value = swap_bits(value, g - 2 + bit, bit)
    sent[:, pl.ds(0, 8)] = value[:n]
    sent[:, pl.ds(8, 8)] = value[n:]
    pl.semaphore_wait(barrier, size - 1 + len(others))
    for other in others:
        pl.semaphore_signal(flag.at[plane], inc=1, device_id=(other * size + place,), device_id_type=MESH)
    value = obs_in[...].reshape(n, 8, 128)
    for major, bit in ((g - 2, 0), (g - 1, 2)):
        value = swap_bits(value, major, bit)
    sent[:, pl.ds(16, 8)] = jnp.stack([value[:half], value[half:]], axis=1).reshape(n, 8, 128)


    def exchange(source, target, send, recv, rows):
        def part(ref, block):
            return ref.at[block, pl.ds(0, rows)]

        def start(to, lower, upper):
            @pl.loop(lower, upper)
            def _(k):
                block = planes[to] * size + inside(size - 1 - k)
                pltpu.make_async_remote_copy(
                    src_ref=part(source, block),
                    dst_ref=part(target, me),
                    send_sem=send.at[planes[to]],
                    recv_sem=recv.at[plane],
                    device_id=(block,),
                    device_id_type=MESH,
                ).start()

        def many(to):
            blocks = pl.ds(planes[to] * size, size - 1 if to == "own" else size)
            return pltpu.make_async_remote_copy(
                src_ref=part(source, blocks),
                dst_ref=part(target, blocks),
                send_sem=send.at[planes[to]],
                recv_sem=recv.at[planes[to]],
                device_id=(me,),
                device_id_type=MESH,
            )

        return start, lambda to: many(to).wait_recv(), lambda: [many(to).wait_send() for to in planes]

    start1, arrive1, depart1 = exchange(sent, held, send1, recv1, 24)
    start2, arrive2, depart2 = exchange(back, landed, send2, recv2, 17)
    start1("far", size - 1, size)
    start1("near", size - 1, size)
    start1("own", 0, size - 1)
    start1("side", size - 1, size)
    for to in ("near", "far", "side"):
        pl.semaphore_wait(flag.at[planes[to]], 1)
        start1(to, 0, size - 1)
    held[me] = sent[me]

    layers, kind_count = angles.shape
    turns = [[half_turn(angles[l, k]) for k in range(kind_count)] for l in range(layers)]
    coefs, shares = [], []
    for l in range(layers):
        row, share = [], []
        for q in range(qubits):
            kind = kinds[l, q]
            is_kind = [jnp.where(kind == k, 1.0, 0.0) for k in range(kind_count)]
            cy = sum(is_kind[k] * turns[l][k][0] for k in range(kind_count - 1))
            sy = sum(is_kind[k] * turns[l][k][1] for k in range(kind_count - 1))
            cz = is_kind[-1] * turns[l][-1][0]
            sz = is_kind[-1] * turns[l][-1][1]
            row.append((cy + is_kind[-1], sy, cz + (1.0 - is_kind[-1]), sz, cy + cz))
            share.append(is_kind)
        coefs.append(row)
        shares.append(share)

    every = range(qubits)
    late = [q for q in every if home[q][0] == MAJOR]
    first, last = min(late), max(late)
    late_edges = [q for q in every if first - 1 <= q <= last]
    early_edges = [q for q in every if q not in late_edges]
    local = [q for q in every if home[q][0] != DEVICE]
    outer = [q for q in every if home[q][0] == DEVICE]
    here = [q for q in every if q not in late]
    ready = [q for q in here if q not in (first - 1, last + 1)]
    rest = [q for q in local if q not in ready]

    for l in range(layers):
        lanes = [
            (coefs[l][q][4], coefs[l][q][1], coefs[l][q][3]) if l == 1 or q in ready else (1.0, 0.0, 0.0)
            for q in range(LANE_BITS)
        ]
        wide[l] = lane_matrix(lanes)

    sums = [[jnp.zeros((8, 128), jnp.float32) for _ in range(kind_count)] for _ in range(layers)]

    def add_terms(l, chosen, place, bra, ket):
        w = minor_sign(SUB, 0) * (bra * other_part(ket))
        w_sum = jnp.sum(w, axis=0)
        for q in chosen:
            y, z = terms(bra, ket, place[q], w, w_sum)
            for k in range(kind_count):
                sums[l][k] = sums[l][k] + shares[l][q][k] * (z if k == kind_count - 1 else y)

    def phase_of(l, chosen, place, edges, majors, chunk, by_matrix):
        turned = {q: coefs[l][q][2:4] for q in chosen if not (by_matrix and place[q][0] == LANE)}
        return phases(place, qubits, edges, majors, me, chunk, turned)

    def turn(x, l, chosen, place, phase, by_matrix=True):
        if by_matrix:
            x = turn_lanes(x, wide.at[l])
        majors = []
        for q in chosen:
            if place[q][0] == MAJOR:
                majors.append((place[q][1], coefs[l][q][0], coefs[l][q][1]))
            elif not (by_matrix and place[q][0] == LANE):
                x = y_gate(x, place[q], coefs[l][q][0], coefs[l][q][1])
        return major_gates(x, majors, phase)

    sign, _ = phases(home, qubits, every, 2 * n, me, 0)
    phase = phase_of(1, local, home, every, 2 * n, 0, True)
    ket = jnp.concatenate([sent[:, pl.ds(0, 8)], sent[:, pl.ds(8, 8)]], 0) * sign
    obs = sent[:, pl.ds(16, 8)]
    bra = scale * jnp.concatenate([weights(obs, 0), weights(obs, 1)], 0) * ket
    add_terms(1, local, home, bra, ket)
    ket, bra = (turn(x, 1, local, home, phase) for x in (ket, bra))
    add_terms(0, local[1:-1], home, bra, ket)

    ready_phase = phase_of(0, ready, away, [], n, 0, True)
    signs = [phases(away, qubits, every, n, me, chunk)[0] for chunk in range(2)]
    mid_phases = [phase_of(1, here, away, early_edges, n, chunk, True) for chunk in range(2)]
    for chunk in range(2):
        flips[chunk] = signs[chunk]
    inner = size.bit_length() - 1
    wide_here = [q for q in here if away[q][0] == MAJOR and away[q][1] >= inner]
    slim_here = [q for q in here if q not in wide_here]
    for origin in ("own", "side", "near", "far"):
        arrive1(origin)
        blocks = pl.ds(planes[origin] * size, size)
        for chunk in range(2):
            ket = held[blocks, pl.ds(8 * chunk, 8)] * flips[chunk, blocks]
            bra = scale * weights(held[blocks, pl.ds(16, 8)], chunk) * ket
            add_terms(1, [q for q in outer if q in slim_here], away, bra, ket)
            begun[chunk, 0, blocks] = ket
            begun[chunk, 1, blocks] = bra
            begun[chunk, 2, blocks] = turn(ket, 1, slim_here, away, None)
            begun[chunk, 3, blocks] = turn(bra, 1, slim_here, away, None)
    for chunk in range(2):
        phase = mid_phases[chunk]
        bra = turn(begun[chunk, 3], 1, wide_here, away, phase, False)
        back[:, pl.ds(8 * chunk, 8)] = turn(bra, 0, ready, away, ready_phase)
        add_terms(1, [q for q in outer if q in wide_here], away, begun[chunk, 1], begun[chunk, 0])
        ket = turn(begun[chunk, 2], 1, wide_here, away, phase, False)
        add_terms(0, [local[-1]] + outer + [0], away, bra, ket)
    spot = [lax.broadcasted_iota(jnp.int32, (8, 128), d) for d in range(2)]
    total = jnp.zeros((8, 128), jnp.float32)
    for l in range(layers):
        for k in range(kind_count):
            row = jnp.sum(sums[l][k], axis=0, keepdims=True)
            total = total + jnp.where(spot[0] == l * kind_count + k, row, 0.0)
    total = jnp.sum(total, axis=1, keepdims=True)
    total = jnp.sum(jnp.where(spot[0] == spot[1], total, 0.0), axis=0, keepdims=True)
    back[:, pl.ds(16, 1)] = jnp.broadcast_to(total, (n, 1, 128))

    start2("far", 0, size)
    start2("near", 0, size)
    start2("side", 0, size)
    start2("own", 0, size - 1)
    landed[me] = back[me]

    late_phase = phase_of(1, late, home, late_edges, 2 * n, 0, False)
    rest_phase = phase_of(0, rest, home, [], 2 * n, 0, False)
    wide_late = [q for q in late if inner <= home[q][1] < g]
    slim = {q: (MAJOR, min(home[q][1], inner)) for q in late if q not in wide_late}
    for origin in ("own", "side", "near", "far"):
        arrive2(origin)
        blocks = pl.ds(planes[origin] * size, size)
        x = jnp.concatenate([landed[blocks, pl.ds(0, 8)], landed[blocks, pl.ds(8, 8)]], 0)
        x = turn(x, 1, list(slim), slim, None, False)
        begun[0, 0, blocks] = x[:size]
        begun[1, 0, blocks] = x[size:]
    x = jnp.concatenate([begun[0, 0], begun[1, 0]], 0)
    x = turn(x, 1, wide_late, home, late_phase, False)
    x = turn(x, 0, rest, home, rest_phase, False)
    for bit in (1, 2):
        x = swap_bits(x, g - 2 + bit, bit)
    out_ref[...] = x.reshape(16 * n, 128)
    grads_ref[...] = jnp.sum(landed[:, pl.ds(16, 1)], axis=0)
    depart1()
    depart2()


def finish(bra_ref, sums_ref, out_ref, grads_ref, picked, sems):
    layers, kind_count = picked.shape
    for l in range(layers):
        picked[pl.ds(l, 1), :] = sums_ref[:, pl.ds(l * kind_count, kind_count)]
    pieces = sems.shape[0] - 1
    rows = out_ref.shape[0] // pieces
    copies = [pltpu.make_async_copy(picked, grads_ref, sems.at[pieces])]
    for k in range(pieces):
        part = pl.ds(k * rows, rows)
        copies.append(pltpu.make_async_copy(bra_ref.at[part], out_ref.at[part], sems.at[k]))
    for copy in copies:
        copy.start()
    for copy in copies:
        copy.wait()


def by_exchange(ket_state, observable, angles, gate_kinds):
    amp_count = ket_state.shape[1]
    n = lax.axis_size("amp")
    qubits = (amp_count * n).bit_length() - 1
    layers, kind_count = angles.shape
    rows = amp_count // 128
    ket = ket_state.reshape(2, rows, 128).transpose(1, 0, 2).reshape(2 * rows, 128)
    vmem = pl.BlockSpec(memory_space=pltpu.VMEM)
    smem = pl.BlockSpec(memory_space=pltpu.SMEM)
    hbm = pl.BlockSpec(memory_space=pltpu.HBM)
    f32 = jnp.float32
    dma = pltpu.SemaphoreType.DMA
    bra, sums = pl.pallas_call(
        functools.partial(kernel, n, qubits),
        out_shape=(
            pltpu.VMEM((2 * rows, 128), f32),
            pltpu.VMEM((1, 128), f32),
        ),
        in_specs=[smem, smem, hbm, hbm],
        out_specs=(vmem, vmem),
        scratch_shapes=[
            pltpu.VMEM((2 * rows, 128), f32),
            pltpu.VMEM((rows, 128), f32),
        ]
        + [pltpu.VMEM((n, 24, 128), f32)] * 4
        + [
            pltpu.SemaphoreType.REGULAR((PLANES,)),
        ]
        + [dma((PLANES,))] * 4
        + [dma((2,)), pltpu.VMEM((layers, 128, 256), f32)]
        + [pltpu.VMEM((2, n, 8, 128), f32), pltpu.VMEM((2, 4, n, 8, 128), f32)],
        compiler_params=pltpu.CompilerParams(
            collective_id=0, has_side_effects=True
        ),
    )(angles, gate_kinds, *(pltpu.with_memory_space_constraint(x, pltpu.HBM) for x in (ket, observable.reshape(rows, 128))))
    out, grads = pl.pallas_call(
        finish,
        out_shape=(
            jax.ShapeDtypeStruct((2 * rows, 128), f32),
            jax.ShapeDtypeStruct((layers, kind_count), f32),
        ),
        in_specs=[vmem, vmem],
        out_specs=(hbm, hbm),
        scratch_shapes=[pltpu.VMEM((layers, kind_count), f32), dma((5,))],
        compiler_params=pltpu.CompilerParams(vmem_limit_bytes=1 << 20),
    )(*(pltpu.with_memory_space_constraint(x, pltpu.VMEM) for x in (bra, sums)))
    bra_state = out.reshape(rows, 2, 128).transpose(1, 0, 2).reshape(2, amp_count)
    return (bra_state, grads)


def per_device(ket_state, observable, angles, gate_kinds):
    tiles = ket_state.shape[1] // (1 << LANE_BITS + SUB_BITS)
    if tiles == lax.axis_size("amp") and tiles >= 8 and angles.shape == (2, 3):
        return by_exchange(ket_state, observable, angles, gate_kinds)
    return on_device(ket_state, observable, angles, gate_kinds)


def solution(mesh):
    placed = (P(None, "amp"), P("amp"), P(), P())
    return jax.shard_map(
        per_device, mesh=mesh, in_specs=placed, out_specs=(P(None, "amp"), P()), check_vma=False
    )
```

```python
import functools
import math

import jax
import jax.numpy as jnp
import numpy as np
from jax import lax
from jax.experimental import pallas as pl
from jax.experimental.pallas import tpu as pltpu
from jax.sharding import PartitionSpec as P

MESH = pl.DeviceIdType.MESH
LANE, SUB, MAJOR, DEVICE, CHUNK = range(5)
LANE_BITS, SUB_BITS = 7, 3
PLANES = 4


def from_partner(value, axis, apart):
    mask = 2**apart
    pairs = [(source, source ^ mask) for source in range(lax.axis_size(axis))]
    return lax.ppermute(value, axis, pairs)


def pair_tables():
    column = np.arange(128)
    flips = []
    signs = []
    for position in range(7):
        upper = column >> position & 1
        flip_table = np.zeros((128, 128), np.float32)
        flip_table[column, column ^ 1 << position] = np.where(upper == 0, -0.5, 0.5)
        flips.append(flip_table)
        signs.append((1 - 2 * upper).astype(np.float32))
    return (np.stack(flips), np.stack(signs))


def layout_map(local_bits, global_bits):
    local_map = list(range(local_bits))
    device_map = [local_bits + bit_num for bit_num in range(global_bits)]
    return (local_map, device_map)


def entangle_sign(local_bits, global_bits, device_id, amp_count):
    local_map, device_map = layout_map(local_bits, global_bits)
    amp_index = lax.iota(jnp.int32, amp_count)
    bit_values = [None] * (local_bits + global_bits)
    for position in range(local_bits):
        bit_values[local_map[position]] = amp_index >> position & 1
    for bit_num in range(global_bits):
        bit_values[device_map[bit_num]] = device_id >> bit_num & 1
    all_bits = local_bits + global_bits
    parity = jnp.zeros((amp_count,), jnp.int32)
    for qubit_id in range(all_bits):
        parity = parity + bit_values[qubit_id] * bit_values[(qubit_id + 1) % all_bits]
    return (1 - 2 * (parity & 1)).astype(jnp.float32)


def rotation_of(angles, gate_kinds, layer_id, qubit_id):
    kind_id = gate_kinds[layer_id, qubit_id]
    chosen = jnp.arange(angles.shape[1]) == kind_id
    rotation = jnp.sum(jnp.where(chosen, angles[layer_id], 0.0))
    return (kind_id, jnp.cos(0.5 * rotation), jnp.sin(0.5 * rotation))


def kind_vector(kind_id, kind_count):
    return (jnp.arange(kind_count) == kind_id).astype(jnp.float32)


def rotate_phase(values, cosine, sine_value):
    return jnp.stack(
        [cosine * values[0] - sine_value * values[1], cosine * values[1] + sine_value * values[0]]
    )


def rotate_position(ket_state, bra_state, position, qubit_id, layer_id, angles, gate_kinds):
    amp_count = ket_state.shape[1]
    fold_shape = (2, amp_count >> position + 1, 2, 1 << position)
    kind_id, cosine, sine_value = rotation_of(angles, gate_kinds, layer_id, qubit_id)

    def turn_y(operands):
        folded_ket, folded_bra = operands
        ket_low, ket_high = (folded_ket[:, :, 0], folded_ket[:, :, 1])
        bra_low, bra_high = (folded_bra[:, :, 0], folded_bra[:, :, 1])
        partial_value = 0.5 * jnp.sum(bra_high * ket_low - bra_low * ket_high)
        new_ket = jnp.stack(
            [cosine * ket_low + sine_value * ket_high, cosine * ket_high - sine_value * ket_low],
            axis=2,
        )
        new_bra = jnp.stack(
            [cosine * bra_low + sine_value * bra_high, cosine * bra_high - sine_value * bra_low],
            axis=2,
        )
        return (new_ket, new_bra, partial_value)

    def turn_z(operands):
        folded_ket, folded_bra = operands
        ket_low, ket_high = (folded_ket[:, :, 0], folded_ket[:, :, 1])
        bra_low, bra_high = (folded_bra[:, :, 0], folded_bra[:, :, 1])
        partial_value = 0.5 * (
            jnp.sum(bra_low[0] * ket_low[1] - bra_low[1] * ket_low[0])
            - jnp.sum(bra_high[0] * ket_high[1] - bra_high[1] * ket_high[0])
        )
        new_ket = jnp.stack(
            [
                rotate_phase(ket_low, cosine, sine_value),
                rotate_phase(ket_high, cosine, -sine_value),
            ],
            axis=2,
        )
        new_bra = jnp.stack(
            [
                rotate_phase(bra_low, cosine, sine_value),
                rotate_phase(bra_high, cosine, -sine_value),
            ],
            axis=2,
        )
        return (new_ket, new_bra, partial_value)

    new_ket, new_bra, partial_value = lax.cond(
        kind_id == 2, turn_z, turn_y, (ket_state.reshape(fold_shape), bra_state.reshape(fold_shape))
    )
    terms = partial_value * kind_vector(kind_id, angles.shape[1])
    return (new_ket.reshape(2, amp_count), new_bra.reshape(2, amp_count), terms)


def contract_rows(left, right):
    return lax.dot_general(
        left,
        right,
        (((0,), (0,)), ((), ())),
        precision=lax.Precision.HIGHEST,
        preferred_element_type=jnp.float32,
    )


def contract_cols(left, right):
    return lax.dot_general(
        left,
        right,
        (((1,), (1,)), ((), ())),
        precision=lax.Precision.HIGHEST,
        preferred_element_type=jnp.float32,
    )


def low_block(ket_state, bra_state, qubit_list, layer_id, angles, gate_kinds):
    amp_count = ket_state.shape[1]
    row_count = amp_count // 128
    flips, signs = pair_tables()
    ket_real = ket_state[0].reshape(row_count, 128)
    ket_imag = ket_state[1].reshape(row_count, 128)
    bra_real = bra_state[0].reshape(row_count, 128)
    bra_imag = bra_state[1].reshape(row_count, 128)
    gram_real = contract_rows(bra_real, ket_real) + contract_rows(bra_imag, ket_imag)
    gram_imag = contract_rows(bra_real, ket_imag) - contract_rows(bra_imag, ket_real)
    gram_diag = jnp.diagonal(gram_imag)
    terms = jnp.zeros((angles.shape[1],), jnp.float32)
    kron_real = None
    kron_imag = None
    for position in range(7):
        kind_id, cosine, sine_value = rotation_of(
            angles, gate_kinds, layer_id, qubit_list[position]
        )
        is_z = kind_id == 2
        partial_value = jnp.where(
            is_z, 0.5 * jnp.sum(signs[position] * gram_diag), jnp.sum(flips[position] * gram_real)
        )
        terms = terms + partial_value * kind_vector(kind_id, angles.shape[1])
        mat_y = jnp.stack([jnp.stack([cosine, sine_value]), jnp.stack([-sine_value, cosine])])
        zero_value = jnp.zeros_like(cosine)
        mat_zr = jnp.stack([jnp.stack([cosine, zero_value]), jnp.stack([zero_value, cosine])])
        mat_zi = jnp.stack(
            [jnp.stack([sine_value, zero_value]), jnp.stack([zero_value, -sine_value])]
        )
        mat_real = jnp.where(is_z, mat_zr, mat_y)
        mat_imag = jnp.where(is_z, mat_zi, jnp.zeros_like(mat_zi))
        if kron_real is None:
            kron_real, kron_imag = (mat_real, mat_imag)
        else:
            kron_real, kron_imag = (
                jnp.kron(mat_real, kron_real) - jnp.kron(mat_imag, kron_imag),
                jnp.kron(mat_real, kron_imag) + jnp.kron(mat_imag, kron_real),
            )

    def apply_block(real_rows, imag_rows):
        new_real = contract_cols(real_rows, kron_real) - contract_cols(imag_rows, kron_imag)
        new_imag = contract_cols(imag_rows, kron_real) + contract_cols(real_rows, kron_imag)
        return jnp.stack([new_real.reshape(amp_count), new_imag.reshape(amp_count)])

    return (apply_block(ket_real, ket_imag), apply_block(bra_real, bra_imag), terms)


def rotate_global(
    ket_state,
    bra_state,
    far_ket,
    far_bra,
    bit_num,
    qubit_id,
    device_id,
    layer_id,
    angles,
    gate_kinds,
):
    kind_id, cosine, sine_value = rotation_of(angles, gate_kinds, layer_id, qubit_id)
    orient = (1 - 2 * (device_id >> bit_num & 1)).astype(jnp.float32)

    def turn_y(operands):
        own_ket, own_bra, other_ket, other_bra = operands
        partial_value = 0.25 * orient * jnp.sum(other_bra * own_ket - own_bra * other_ket)
        return (
            cosine * own_ket + orient * sine_value * other_ket,
            cosine * own_bra + orient * sine_value * other_bra,
            partial_value,
        )

    def turn_z(operands):
        own_ket, own_bra, other_ket, other_bra = operands
        partial_value = 0.5 * orient * jnp.sum(own_bra[0] * own_ket[1] - own_bra[1] * own_ket[0])
        return (
            rotate_phase(own_ket, cosine, orient * sine_value),
            rotate_phase(own_bra, cosine, orient * sine_value),
            partial_value,
        )

    new_ket, new_bra, partial_value = lax.cond(
        kind_id == 2, turn_z, turn_y, (ket_state, bra_state, far_ket, far_bra)
    )
    return (new_ket, new_bra, partial_value * kind_vector(kind_id, angles.shape[1]))


def on_device(ket_state, observable, angles, gate_kinds):
    amp_count = ket_state.shape[1]
    local_bits = amp_count.bit_length() - 1
    group_size = lax.axis_size("amp")
    global_bits = group_size.bit_length() - 1
    device_id = lax.axis_index("amp")
    layer_count = angles.shape[0]
    kind_count = angles.shape[1]
    bra_state = 2.0 / math.sqrt(amp_count * group_size) * observable[None, :] * ket_state
    sign_cache = {}
    grads_local = jnp.zeros((layer_count, kind_count), jnp.float32)
    for sweep_id in range(layer_count):
        layer_id = layer_count - 1 - sweep_id
        layout = 0
        local_map, device_map = layout_map(local_bits, global_bits)
        if layout not in sign_cache:
            sign_cache[layout] = entangle_sign(local_bits, global_bits, device_id, amp_count)
        phase_sign = sign_cache[layout]
        ket_state = ket_state * phase_sign[None, :]
        bra_state = bra_state * phase_sign[None, :]
        ket_state, bra_state, layer_terms = low_block(
            ket_state, bra_state, local_map[:7], layer_id, angles, gate_kinds
        )
        for position in range(7, local_bits):
            ket_state, bra_state, partial_value = rotate_position(
                ket_state, bra_state, position, local_map[position], layer_id, angles, gate_kinds
            )
            layer_terms = layer_terms + partial_value
        for bit_num in range(global_bits):
            far_ket, far_bra = from_partner((ket_state, bra_state), "amp", bit_num)
            ket_state, bra_state, partial_value = rotate_global(
                ket_state,
                bra_state,
                far_ket,
                far_bra,
                bit_num,
                device_map[bit_num],
                device_id,
                layer_id,
                angles,
                gate_kinds,
            )
            layer_terms = layer_terms + partial_value
        grads_local = grads_local.at[layer_id].set(layer_terms)
    grads = lax.psum(grads_local, "amp")
    return (bra_state, grads)


def chunk_layouts(g):
    top = g + LANE_BITS + SUB_BITS - 1
    home, away = {}, {}
    for q in range(LANE_BITS):
        home[q] = away[q] = (LANE, q)
    for bit, q in ((1, top - 1), (2, top)):
        home[q] = away[q] = (SUB, bit)
    moved = list(range(LANE_BITS + 2, top - 1)) + [LANE_BITS]
    for bit, q in enumerate(moved):
        home[q], away[q] = (MAJOR, bit), (DEVICE, bit)
    home[LANE_BITS + 1], away[LANE_BITS + 1] = (MAJOR, g), (CHUNK, 0)
    for bit in range(g):
        home[top + 1 + bit], away[top + 1 + bit] = (DEVICE, bit), (MAJOR, bit)
    return home, away


def split_major(x, bit):
    fold = x.reshape((x.shape[0] >> bit + 1, 2, 1 << bit) + x.shape[1:])
    return fold[:, 0], fold[:, 1]


def join_major(x0, x1):
    out = jnp.stack([x0, x1], axis=1)
    return out.reshape((-1,) + out.shape[3:])


def minor_bit(axis, bit):
    return lax.broadcasted_iota(jnp.int32, (1, 8, 128), 1 if axis == SUB else 2) >> bit & 1


def minor_sign(axis, bit):
    return (1 - 2 * minor_bit(axis, bit)).astype(jnp.float32)


def shifted(x, axis, by):
    dim = 1 if axis == SUB else 2
    return pltpu.roll(x, by % x.shape[dim], dim)


def partner(x, axis, bit):
    step = 1 << bit
    up = shifted(x, axis, -step)
    if 2 * step == x.shape[1 if axis == SUB else 2]:
        return up
    return jnp.where(minor_bit(axis, bit) == 0, up, shifted(x, axis, step))


def swap_bits(x, major, sub):
    x0, x1 = split_major(x, major)
    lower = minor_bit(SUB, sub) == 0

    def roll3(y, by):
        z = y.reshape((-1,) + y.shape[2:])
        return shifted(z, SUB, by).reshape(y.shape)

    step = 1 << sub
    return join_major(jnp.where(lower, x0, roll3(x1, step)), jnp.where(lower, roll3(x0, -step), x1))


def other_part(x):
    return partner(x, SUB, 0)


def weights(obs, chunk):
    place = lax.broadcasted_iota(jnp.int32, (1, 8, 128), 1) & 3
    if chunk == 0:
        end, far = 0, 3
    else:
        end, far = 3, 0
    step = 1 if chunk == 0 else -1
    near = jnp.where(place == end, obs, shifted(obs, SUB, step))
    return jnp.where(place == far, shifted(obs, SUB, 2 * step), near)


def y_gate(x, place, cy, sy):
    axis, bit = place
    if axis == MAJOR:
        x0, x1 = split_major(x, bit)
        return join_major(cy * x0 + sy * x1, cy * x1 - sy * x0)
    return cy * x + (sy * minor_sign(axis, bit)) * partner(x, axis, bit)


def major_gates(x, gates, phase):
    tiles = [x[i : i + 1] for i in range(x.shape[0])]
    split = (len(gates) + 1) // 2 if len(gates) > 3 else len(gates)
    passes = [p for p in (gates[:split], gates[split:]) if p]
    for number, some in enumerate(passes):
        spread = sum(1 << bit for bit, _, _ in some)
        for base in range(len(tiles)):
            if base & spread:
                continue
            group = [base]
            for bit, _, _ in some:
                group = group + [i + (1 << bit) for i in group]
            for bit, cy, sy in some:
                for i in group:
                    if not i >> bit & 1:
                        j = i + (1 << bit)
                        a, b = tiles[i], tiles[j]
                        tiles[i], tiles[j] = cy * a + sy * b, cy * b - sy * a
            if phase is not None and number == len(passes) - 1:
                for i in group:
                    tiles[i] = phase[0][i : i + 1] * tiles[i] + phase[1][i : i + 1] * other_part(tiles[i])
    return jnp.concatenate(tiles, 0)


def lane_matrix(coefs):
    at = [lax.broadcasted_iota(jnp.int32, (128, 128), d) for d in range(2)]
    re, im = None, None
    for bit, (c, sy, sz) in enumerate(coefs):
        old, new = (x >> bit & 1 for x in at)
        z = (1 - 2 * new).astype(jnp.float32)
        same = old == new
        a, b = jnp.where(same, c, sy * z), jnp.where(same, sz * z, 0.0)
        re, im = (a, b) if re is None else (re * a - im * b, re * b + im * a)
    return jnp.concatenate([re, im], 1)


def turn_lanes(x, matrix):
    both = lax.dot_general(
        x.reshape(-1, 128),
        matrix[...],
        (((1,), (0,)), ((), ())),
        precision=lax.Precision.HIGH,
        preferred_element_type=jnp.float32,
    )
    re, im = both[:, :128].reshape(x.shape), both[:, 128:].reshape(x.shape)
    return re - minor_sign(SUB, 0) * other_part(im)


def terms(bra, ket, place, w, w_sum):
    axis, bit = place
    if axis == MAJOR:
        b0, b1 = split_major(bra, bit)
        k0, k1 = split_major(ket, bit)
        w0, w1 = split_major(w, bit)
        return 0.5 * jnp.sum(b1 * k0 - b0 * k1, axis=(0, 1)), 0.5 * jnp.sum(w0 - w1, axis=(0, 1))
    z = 0.5 * minor_sign(axis, bit)[0]
    return -z * jnp.sum(bra * partner(ket, axis, bit), axis=0), z * w_sum


def phases(place, qubits, edges, majors, me, chunk, turns=None):
    def bit_of(q):
        axis, bit = place[q]
        if axis in (LANE, SUB):
            return minor_bit(axis, bit)
        return me >> bit & 1 if axis == DEVICE else chunk

    at_major = {place[q][1]: q for q in range(qubits) if place[q][0] == MAJOR}
    parity = jnp.zeros((1, 8, 128), jnp.int32)
    for q in edges:
        ends = (q, (q + 1) % qubits)
        if all(place[e][0] != MAJOR for e in ends):
            parity = parity + bit_of(ends[0]) * bit_of(ends[1])
    re = (1 - 2 * (parity & 1)).astype(jnp.float32)
    im = None

    def times(re, im, c, s):
        if im is None:
            return re * c, re * s
        return re * c - im * s, im * c + re * s

    turns = turns or {}
    for q, (c, s) in turns.items():
        axis, bit = place[q]
        if axis != MAJOR:
            re, im = times(re, im, c, s * minor_sign(axis, bit))
    for j in range(majors.bit_length() - 1):
        q = at_major[j]
        parity, flips = None, []
        for edge, o in ((q, (q + 1) % qubits), ((q - 1) % qubits, (q - 1) % qubits)):
            if edge not in edges:
                continue
            if place[o][0] != MAJOR:
                parity = bit_of(o) if parity is None else parity + bit_of(o)
            elif place[o][1] < j:
                flips.append(place[o][1])

        def upper(x):
            if parity is not None:
                x = x * jnp.broadcast_to(1 - 2 * (parity & 1), (1, 8, 128)).astype(jnp.float32)
            for bit in flips:
                x0, x1 = split_major(x, bit)
                x = join_major(x0, -x1)
            return x

        lo, hi = (re, im), (upper(re), None if im is None else upper(im))
        if q in turns:
            c, s = turns[q]
            lo, hi = times(*lo, c, s), times(*hi, c, -s)
        re = jnp.concatenate([lo[0], hi[0]], 0)
        im = None if lo[1] is None else jnp.concatenate([lo[1], hi[1]], 0)
    return (re, None) if im is None else (re, -minor_sign(SUB, 0) * im)


def half_turn(angle):
    x = 0.5 * angle
    x2 = x * x
    cosine, sine = 0.0, 0.0
    for n in range(8, -1, -1):
        cosine = cosine * x2 + (-1.0) ** n / math.factorial(2 * n)
        sine = sine * x2 + (-1.0) ** n / math.factorial(2 * n + 1)
    return cosine, sine * x


def kernel(
    n, qubits, angles, kinds, ket_ref, obs_ref, out_ref, grads_ref,
    ket_in, obs_in, sent, held, back, landed,
    flag, send1, recv1, send2, recv2, load, wide, flips, begun,
):
    me = lax.axis_index("amp")
    g = n.bit_length() - 1
    home, away = chunk_layouts(g)
    scale = 2.0 / math.sqrt(2**qubits)

    loads = [
        pltpu.make_async_copy(ket_ref, ket_in, load.at[0]),
        pltpu.make_async_copy(obs_ref, obs_in, load.at[1]),
    ]
    for copy in loads:
        copy.start()

    half, size = n // 2, n // PLANES
    plane, place = me // size, me % size
    upper = plane // 2
    near = 2 - upper
    far = near + 1 - 2 * upper
    side = plane + 1 - 2 * (plane % 2)
    others = (near, far, side)
    planes = {"far": far, "near": near, "side": side, "own": plane}

    def inside(j):
        spot = place + j
        for bit in range(size.bit_length() - 1):
            step = 1 << bit
            spot = spot - 2 * step * (place // step % 2) * (j // step % 2)
        return spot

    barrier = pltpu.get_barrier_semaphore()
    for other in others:
        pl.semaphore_signal(barrier, inc=1, device_id=(other * size + place,), device_id_type=MESH)
    for j in range(1, size):
        pl.semaphore_signal(barrier, inc=1, device_id=(plane * size + inside(j),), device_id_type=MESH)
    for copy in loads:
        copy.wait()

    value = ket_in[...].reshape(2 * n, 8, 128)
    for bit in (1, 2):
        value = swap_bits(value, g - 2 + bit, bit)
    sent[:, pl.ds(0, 8)] = value[:n]
    sent[:, pl.ds(8, 8)] = value[n:]
    pl.semaphore_wait(barrier, size - 1 + len(others))
    for other in others:
        pl.semaphore_signal(flag.at[plane], inc=1, device_id=(other * size + place,), device_id_type=MESH)
    value = scale * obs_in[...].reshape(n, 8, 128)
    for major, bit in ((g - 2, 0), (g - 1, 2)):
        value = swap_bits(value, major, bit)
    sent[:, pl.ds(16, 8)] = jnp.stack([value[:half], value[half:]], axis=1).reshape(n, 8, 128)


    def exchange(source, target, send, recv, rows):
        def part(ref, block):
            return ref.at[block, pl.ds(0, rows)]

        def start(to, lower, upper):
            @pl.loop(lower, upper)
            def _(k):
                block = planes[to] * size + inside(size - 1 - k)
                pltpu.make_async_remote_copy(
                    src_ref=part(source, block),
                    dst_ref=part(target, me),
                    send_sem=send.at[planes[to]],
                    recv_sem=recv.at[plane],
                    device_id=(block,),
                    device_id_type=MESH,
                ).start()

        def many(to):
            blocks = pl.ds(planes[to] * size, size - 1 if to == "own" else size)
            return pltpu.make_async_remote_copy(
                src_ref=part(source, blocks),
                dst_ref=part(target, blocks),
                send_sem=send.at[planes[to]],
                recv_sem=recv.at[planes[to]],
                device_id=(me,),
                device_id_type=MESH,
            )

        return start, lambda to: many(to).wait_recv(), lambda: [many(to).wait_send() for to in planes]

    start1, arrive1, depart1 = exchange(sent, held, send1, recv1, 24)
    start2, arrive2, depart2 = exchange(back, landed, send2, recv2, 17)
    start1("far", size - 1, size)
    start1("near", size - 1, size)
    start1("own", 0, size - 1)
    start1("side", size - 1, size)
    for to in ("near", "far", "side"):
        pl.semaphore_wait(flag.at[planes[to]], 1)
        start1(to, 0, size - 1)
    held[me] = sent[me]

    layers, kind_count = angles.shape
    turns = [[half_turn(angles[l, k]) for k in range(kind_count)] for l in range(layers)]
    coefs, shares = [], []
    for l in range(layers):
        row, share = [], []
        for q in range(qubits):
            kind = kinds[l, q]
            is_kind = [jnp.where(kind == k, 1.0, 0.0) for k in range(kind_count)]
            cy = sum(is_kind[k] * turns[l][k][0] for k in range(kind_count - 1))
            sy = sum(is_kind[k] * turns[l][k][1] for k in range(kind_count - 1))
            cz = is_kind[-1] * turns[l][-1][0]
            sz = is_kind[-1] * turns[l][-1][1]
            row.append((cy + is_kind[-1], sy, cz + (1.0 - is_kind[-1]), sz, cy + cz))
            share.append(is_kind)
        coefs.append(row)
        shares.append(share)

    every = range(qubits)
    late = [q for q in every if home[q][0] == MAJOR]
    first, last = min(late), max(late)
    late_edges = [q for q in every if first - 1 <= q <= last]
    early_edges = [q for q in every if q not in late_edges]
    local = [q for q in every if home[q][0] != DEVICE]
    outer = [q for q in every if home[q][0] == DEVICE]
    here = [q for q in every if q not in late]
    ready = [q for q in here if q not in (first - 1, last + 1)]
    rest = [q for q in local if q not in ready]

    for l in range(layers):
        lanes = [
            (coefs[l][q][4], coefs[l][q][1], coefs[l][q][3]) if l == 1 or q in ready else (1.0, 0.0, 0.0)
            for q in range(LANE_BITS)
        ]
        wide[l] = lane_matrix(lanes)

    sums = [[jnp.zeros((8, 128), jnp.float32) for _ in range(kind_count)] for _ in range(layers)]

    def add_terms(l, chosen, place, bra, ket):
        w = minor_sign(SUB, 0) * (bra * other_part(ket))
        w_sum = jnp.sum(w, axis=0)
        for q in chosen:
            y, z = terms(bra, ket, place[q], w, w_sum)
            for k in range(kind_count):
                sums[l][k] = sums[l][k] + shares[l][q][k] * (z if k == kind_count - 1 else y)

    def phase_of(l, chosen, place, edges, majors, chunk, by_matrix):
        turned = {q: coefs[l][q][2:4] for q in chosen if not (by_matrix and place[q][0] == LANE)}
        return phases(place, qubits, edges, majors, me, chunk, turned)

    def turn(x, l, chosen, place, phase, by_matrix=True):
        if by_matrix:
            x = turn_lanes(x, wide.at[l])
        majors = []
        for q in chosen:
            if place[q][0] == MAJOR:
                majors.append((place[q][1], coefs[l][q][0], coefs[l][q][1]))
            elif not (by_matrix and place[q][0] == LANE):
                x = y_gate(x, place[q], coefs[l][q][0], coefs[l][q][1])
        return major_gates(x, majors, phase)

    sign, _ = phases(home, qubits, every, 2 * n, me, 0)
    phase = phase_of(1, local, home, every, 2 * n, 0, True)
    ket = jnp.concatenate([sent[:, pl.ds(0, 8)], sent[:, pl.ds(8, 8)]], 0) * sign
    obs = sent[:, pl.ds(16, 8)]
    bra = jnp.concatenate([weights(obs, 0), weights(obs, 1)], 0) * ket
    add_terms(1, local, home, bra, ket)
    ket, bra = (turn(x, 1, local, home, phase) for x in (ket, bra))
    add_terms(0, local[1:-1], home, bra, ket)

    ready_phase = phase_of(0, ready, away, [], n, 0, True)
    signs = [phases(away, qubits, every, n, me, chunk)[0] for chunk in range(2)]
    mid_phases = [phase_of(1, here, away, early_edges, n, chunk, True) for chunk in range(2)]
    for chunk in range(2):
        flips[chunk] = signs[chunk]
    inner = size.bit_length() - 1
    wide_here = [q for q in here if away[q][0] == MAJOR and away[q][1] >= inner]
    slim_here = [q for q in here if q not in wide_here]
    for origin in ("own", "side", "near", "far"):
        arrive1(origin)
        blocks = pl.ds(planes[origin] * size, size)
        for chunk in range(2):
            ket = held[blocks, pl.ds(8 * chunk, 8)] * flips[chunk, blocks]
            bra = weights(held[blocks, pl.ds(16, 8)], chunk) * ket
            add_terms(1, [q for q in outer if q in slim_here], away, bra, ket)
            begun[chunk, 0, blocks] = ket
            begun[chunk, 1, blocks] = bra
            begun[chunk, 2, blocks] = turn(ket, 1, slim_here, away, None)
            begun[chunk, 3, blocks] = turn(bra, 1, slim_here, away, None)
    for chunk in range(2):
        phase = mid_phases[chunk]
        bra = turn(begun[chunk, 3], 1, wide_here, away, phase, False)
        back[:, pl.ds(8 * chunk, 8)] = turn(bra, 0, ready, away, ready_phase)
        add_terms(1, [q for q in outer if q in wide_here], away, begun[chunk, 1], begun[chunk, 0])
        ket = turn(begun[chunk, 2], 1, wide_here, away, phase, False)
        add_terms(0, [local[-1]] + outer + [0], away, bra, ket)
    spot = [lax.broadcasted_iota(jnp.int32, (8, 128), d) for d in range(2)]
    total = jnp.zeros((8, 128), jnp.float32)
    for l in range(layers):
        for k in range(kind_count):
            row = jnp.sum(sums[l][k], axis=0, keepdims=True)
            total = total + jnp.where(spot[0] == l * kind_count + k, row, 0.0)
    total = jnp.sum(total, axis=1, keepdims=True)
    total = jnp.sum(jnp.where(spot[0] == spot[1], total, 0.0), axis=0, keepdims=True)
    back[:, pl.ds(16, 1)] = jnp.broadcast_to(total, (n, 1, 128))

    start2("far", 0, size)
    start2("near", 0, size)
    start2("side", 0, size)
    start2("own", 0, size - 1)
    landed[me] = back[me]

    late_phase = phase_of(1, late, home, late_edges, 2 * n, 0, False)
    rest_phase = phase_of(0, rest, home, [], 2 * n, 0, False)
    wide_late = [q for q in late if inner <= home[q][1] < g]
    slim = {q: (MAJOR, min(home[q][1], inner)) for q in late if q not in wide_late}
    for origin in ("own", "side", "near", "far"):
        arrive2(origin)
        blocks = pl.ds(planes[origin] * size, size)
        x = jnp.concatenate([landed[blocks, pl.ds(0, 8)], landed[blocks, pl.ds(8, 8)]], 0)
        x = turn(x, 1, list(slim), slim, None, False)
        begun[0, 0, blocks] = x[:size]
        begun[1, 0, blocks] = x[size:]
    x = jnp.concatenate([begun[0, 0], begun[1, 0]], 0)
    x = turn(x, 1, wide_late, home, late_phase, False)
    x = turn(x, 0, rest, home, rest_phase, False)
    for bit in (1, 2):
        x = swap_bits(x, g - 2 + bit, bit)
    out_ref[...] = x.reshape(16 * n, 128)
    grads_ref[...] = jnp.sum(landed[:, pl.ds(16, 1)], axis=0)
    depart1()
    depart2()


def finish(bra_ref, sums_ref, out_ref, grads_ref, picked, sems):
    layers, kind_count = picked.shape
    for l in range(layers):
        picked[pl.ds(l, 1), :] = sums_ref[:, pl.ds(l * kind_count, kind_count)]
    pieces = sems.shape[0] - 1
    rows = out_ref.shape[0] // pieces
    copies = [pltpu.make_async_copy(picked, grads_ref, sems.at[pieces])]
    for k in range(pieces):
        part = pl.ds(k * rows, rows)
        copies.append(pltpu.make_async_copy(bra_ref.at[part], out_ref.at[part], sems.at[k]))
    for copy in copies:
        copy.start()
    for copy in copies:
        copy.wait()


def by_exchange(ket_state, observable, angles, gate_kinds):
    amp_count = ket_state.shape[1]
    n = lax.axis_size("amp")
    qubits = (amp_count * n).bit_length() - 1
    layers, kind_count = angles.shape
    rows = amp_count // 128
    ket = ket_state.reshape(2, rows, 128).transpose(1, 0, 2).reshape(2 * rows, 128)
    vmem = pl.BlockSpec(memory_space=pltpu.VMEM)
    smem = pl.BlockSpec(memory_space=pltpu.SMEM)
    hbm = pl.BlockSpec(memory_space=pltpu.HBM)
    f32 = jnp.float32
    dma = pltpu.SemaphoreType.DMA
    bra, sums = pl.pallas_call(
        functools.partial(kernel, n, qubits),
        out_shape=(
            pltpu.VMEM((2 * rows, 128), f32),
            pltpu.VMEM((1, 128), f32),
        ),
        in_specs=[smem, smem, hbm, hbm],
        out_specs=(vmem, vmem),
        scratch_shapes=[
            pltpu.VMEM((2 * rows, 128), f32),
            pltpu.VMEM((rows, 128), f32),
        ]
        + [pltpu.VMEM((n, 24, 128), f32)] * 4
        + [
            pltpu.SemaphoreType.REGULAR((PLANES,)),
        ]
        + [dma((PLANES,))] * 4
        + [dma((2,)), pltpu.VMEM((layers, 128, 256), f32)]
        + [pltpu.VMEM((2, n, 8, 128), f32), pltpu.VMEM((2, 4, n, 8, 128), f32)],
        compiler_params=pltpu.CompilerParams(
            collective_id=0, has_side_effects=True
        ),
    )(angles, gate_kinds, *(pltpu.with_memory_space_constraint(x, pltpu.HBM) for x in (ket, observable.reshape(rows, 128))))
    out, grads = pl.pallas_call(
        finish,
        out_shape=(
            jax.ShapeDtypeStruct((2 * rows, 128), f32),
            jax.ShapeDtypeStruct((layers, kind_count), f32),
        ),
        in_specs=[vmem, vmem],
        out_specs=(hbm, hbm),
        scratch_shapes=[pltpu.VMEM((layers, kind_count), f32), dma((5,))],
        compiler_params=pltpu.CompilerParams(vmem_limit_bytes=1 << 20),
    )(*(pltpu.with_memory_space_constraint(x, pltpu.VMEM) for x in (bra, sums)))
    bra_state = out.reshape(rows, 2, 128).transpose(1, 0, 2).reshape(2, amp_count)
    return (bra_state, grads)


def per_device(ket_state, observable, angles, gate_kinds):
    tiles = ket_state.shape[1] // (1 << LANE_BITS + SUB_BITS)
    if tiles == lax.axis_size("amp") and tiles >= 8 and angles.shape == (2, 3):
        return by_exchange(ket_state, observable, angles, gate_kinds)
    return on_device(ket_state, observable, angles, gate_kinds)


def solution(mesh):
    placed = (P(None, "amp"), P("amp"), P(), P())
    return jax.shard_map(
        per_device, mesh=mesh, in_specs=placed, out_specs=(P(None, "amp"), P()), check_vma=False
    )
```
